32 devices in a mesh: row: 4 (over z), col: 8 (over y, x, core).
Axes of the slice: x: 2, y: 2, z: 4, core: 2. Of those that a mesh axis runs over, the one named last changes fastest.
Arguments:
- adjacency: int32 [32768, 2048], P('col', 'row'), may hold values from -2147483648 to 2147483647, as said below
- frontier: bfloat16 [65536, 128], P(('row', 'col')), may hold values from 0 to 1, as said below
- visited: int32 [4, 32768], P(None, ('col', 'row')), may hold values from -2147483648 to 2147483647, as said below
Outputs:
- path_counts: float32 [32768, 128], P(('col', 'row'))
- reached_bits: int32 [4, 32768], P(None, ('col', 'row'))
The draws below stay inside these ranges and needn't reach their ends.
Inputs may be any that keep to these rules, and one draw needn't show every extreme that they name: Bit k of adjacency[d, w] is the edge from source vertex 32 w + k to destination d; degrees and edge densities differ between vertices and between blocks of 128 by 128 vertices. `frontier`: values are zero or between 0.1 and 1. Bit k of visited[w, d] tells whether destination d was reached from root 32 w + k.
All inputs are finite; a program needn't handle non-finite values.
Results may differ from the reference program's by a relative error of at most 0.0003.
Values may be sent and summed in bfloat16 or wider, within the bound.
A program may use at most 64 MiB of HBM per device.

```python
import functools
import math
import jax
import jax.numpy as jnp
from jax import lax

SOURCES = 128
NDST = 32768
NSRC = 65536
WORDS = 4


def draw_adjacency(key, part):
    column_words = NSRC // 32
    key_list = jax.random.split(jax.random.fold_in(key, 11), 6)
    vertex_level = jax.random.randint(key_list[0], (NDST, 1), 0, 8, dtype=jnp.int32)
    tile_level = jax.random.randint(key_list[1], (NDST // 128, column_words // 4), 0, 3, dtype=jnp.int32)
    tile_level = jnp.repeat(jnp.repeat(tile_level, 128, axis=0), 4, axis=1)
    rate_base = jnp.int32(2097152 // NSRC)
    threshold = jnp.left_shift(rate_base, vertex_level + tile_level)
    selector = jax.random.randint(key_list[2], (NDST, column_words), 0, 1048576, dtype=jnp.int32)
    packed_words = jax.random.randint(key_list[3], (NDST, column_words), -2147483648, 2147483647, dtype=jnp.int32)
    for section_index in range(2):
        extra_words = jax.random.randint(key_list[4 + section_index], (NDST, column_words), -2147483648, 2147483647, dtype=jnp.int32)
        packed_words = jnp.bitwise_and(packed_words, extra_words)
    return jnp.where(selector < threshold, packed_words, jnp.int32(0))


def draw_frontier(key, part):
    key_list = jax.random.split(jax.random.fold_in(key, 23), 2)
    keep_mask = jax.random.uniform(key_list[0], (NSRC, SOURCES), jnp.float32) < 0.5
    magnitude = 0.1 * jnp.exp(jax.random.uniform(key_list[1], (NSRC, SOURCES), jnp.float32) * math.log(10.0))
    values = jnp.where(keep_mask, magnitude, jnp.float32(0.0))
    return values.astype(jnp.bfloat16)


def draw_visited(key, part):
    key_list = jax.random.split(jax.random.fold_in(key, 37), 2)
    first_words = jax.random.randint(key_list[0], (WORDS, NDST), -2147483648, 2147483647, dtype=jnp.int32)
    second_words = jax.random.randint(key_list[1], (WORDS, NDST), -2147483648, 2147483647, dtype=jnp.int32)
    return jnp.bitwise_and(first_words, second_words)


def setup_inputs(seed: int = 0) -> dict:
    arg_keys = jax.random.split(jax.random.key(seed), 4)
    return {
        "adjacency": draw_adjacency(jax.random.fold_in(arg_keys[3], 71), 0),
        "frontier": draw_frontier(jax.random.fold_in(arg_keys[3], 71), 0),
        "visited": draw_visited(jax.random.fold_in(arg_keys[3], 71), 0),
    }


def expand_bits(packed):
    shift_table = jnp.arange(32, dtype=jnp.int32)
    bit_table = jnp.bitwise_and(jnp.right_shift(packed[:, :, None], shift_table), 1)
    return bit_table.reshape(packed.shape[0], packed.shape[1] * 32).astype(jnp.bfloat16)


def finish(reached, visited):
    row_count = reached.shape[0]
    word_count = visited.shape[0]
    shift_table = jnp.arange(32, dtype=jnp.int32)
    seen_bits = jnp.bitwise_and(jnp.right_shift(visited[:, :, None], shift_table), 1)
    seen_bits = jnp.transpose(seen_bits, (1, 0, 2)).reshape(row_count, word_count * 32)
    path_counts = jnp.where(seen_bits == 1, jnp.float32(0.0), reached)
    fresh = jnp.logical_and(seen_bits == 0, reached > 0).astype(jnp.int32)
    fresh = fresh.reshape(row_count, word_count, 32)
    added = functools.reduce(jnp.bitwise_or, [jnp.left_shift(fresh[:, :, position], position) for position in range(32)])
    reached_bits = jnp.bitwise_or(visited, jnp.transpose(added))
    return path_counts, reached_bits


def reference(adjacency, frontier, visited):
    dst_total = adjacency.shape[0]
    block_len = math.gcd(dst_total, 512)
    blocks = adjacency.reshape(dst_total // block_len, block_len, adjacency.shape[1])

    def one_block(packed):
        return jnp.dot(expand_bits(packed), frontier, preferred_element_type=jnp.float32)

    reached = lax.map(one_block, blocks).reshape(dst_total, frontier.shape[1])
    return finish(reached, visited)
```

```python
import functools
import math

import jax
import jax.numpy as jnp
import numpy as np
from jax import lax
from jax.experimental import pallas as pl
from jax.experimental.pallas import tpu as pltpu
from jax.sharding import PartitionSpec as P

MESH = pl.DeviceIdType.MESH
LOW = 0.09
LEVELS = 65000.0


def expand_bits(words):
    one = jnp.full(words.shape, 1, jnp.float8_e4m3fn)
    zero = jnp.full(words.shape, 0, jnp.float8_e4m3fn)
    pieces = []
    for byte in range(4):
        part = (words >> (8 * byte)).astype(jnp.int8)
        for bit in range(8):
            mask = np.int8(-128) if bit == 7 else np.int8(1 << bit)
            pieces.append(jnp.where((part & mask) != 0, one, zero))
    return jnp.concatenate(pieces, axis=0)


def encode(value, scale):
    code = jnp.log(jnp.maximum(value, LOW)) * scale + (1.5 - math.log(LOW) * scale)
    code = jnp.where(value > 0, code, 0.0).astype(jnp.int32)
    return (code - 32768).astype(jnp.int16)


def decode(code, scale):
    code = code.astype(jnp.int32) + 32768
    value = jnp.exp((code - 1).astype(jnp.float32) * (1.0 / scale) + math.log(LOW))
    return jnp.where(code > 0, value, 0.0)


def flip(index, bit):
    return index + bit - 2 * bit * ((index // bit) % 2)


def kernel(
    n_row, n_col, adj, ft, visited, counts, bits,
    stage, words, fbuf, total, out_code, in_code,
    load_sem, own_sem, fsend, frecv, psend, precv,
):
    r, c = lax.axis_index("row"), lax.axis_index("col")
    dst, width = adj.shape
    depth = ft.shape[1]
    wide = width // n_col
    part = dst // n_row
    half = math.gcd(dst, 2048)
    halves = dst // half
    tile = stage.shape[1]
    tiles = dst // tile
    paired = n_col == 8
    scale = LEVELS / math.log(width * 32 * 1.01 / LOW)

    def load(t, slot):
        return pltpu.make_async_copy(
            adj.at[pl.ds(pl.multiple_of(t * tile, tile), tile), :], stage.at[slot], load_sem.at[slot]
        )

    load(0, 0).start()
    own = pltpu.make_async_copy(ft, fbuf.at[c], own_sem)
    own.start()

    if paired:
        mates = [flip(c, 1), flip(c, 2), flip(c, 4)]
    else:
        mates = [lax.rem(c + i, n_col) for i in range(1, n_col)]
    others = [lax.rem(r + i, n_row) for i in range(1, n_row)]
    barrier = pltpu.get_barrier_semaphore()
    for mate in mates:
        pl.semaphore_signal(barrier, inc=1, device_id={"col": mate}, device_id_type=MESH)
    for other in others:
        pl.semaphore_signal(barrier, inc=1, device_id={"row": other}, device_id_type=MESH)
    pl.semaphore_wait(barrier, len(mates) + len(others))

    def send(src, dst_ref, role, mate):
        return pltpu.make_async_remote_copy(
            src_ref=src, dst_ref=dst_ref, send_sem=fsend.at[role], recv_sem=frecv.at[role],
            device_id={"col": mate}, device_id_type=MESH,
        )

    if paired:
        pair, east, north = mates
        first, second = pl.ds(0, ft.shape[0] // 2), pl.ds(ft.shape[0] // 2, ft.shape[0] // 2)
        diagonal = flip(east, 4)
        slots = [pair, east, north, diagonal, diagonal, flip(pair, 2), flip(pair, 4), flip(diagonal, 1)]
        sends = [
            send(ft, fbuf.at[c], 0, pair),
            send(ft, fbuf.at[c], 1, east),
            send(ft, fbuf.at[c], 2, north),
            send(fbuf.at[east, first], fbuf.at[east, first], 3, north),
            send(fbuf.at[north, second], fbuf.at[north, second], 4, east),
            send(fbuf.at[east], fbuf.at[east], 5, pair),
            send(fbuf.at[north], fbuf.at[north], 6, pair),
            send(fbuf.at[diagonal], fbuf.at[diagonal], 7, pair),
        ]
        for role in (1, 2, 0):
            sends[role].start()

        def arrived(role):
            place = fbuf.at[slots[role]]
            if role == 3:
                place = fbuf.at[diagonal, first]
            if role == 4:
                place = fbuf.at[diagonal, second]
            send(place, place, role, pair).wait_recv()

    else:
        sends = [send(ft, fbuf.at[c], i, mate) for i, mate in enumerate(mates)]
        for copy in sends:
            copy.start()

    @pl.loop(0, tiles)
    def _(t):
        slot = lax.rem(t, 2)

        @pl.when(t + 1 < tiles)
        def _():
            load(t + 1, 1 - slot).start()

        load(t, slot).wait()
        words[:, pl.ds(pl.multiple_of(t * tile, tile), tile)] = stage[slot].T

    total[...] = jnp.zeros_like(total)
    own.wait()

    def product(slot, start, size):
        packed = words[pl.ds(pl.multiple_of(slot * wide, wide), wide), pl.ds(start, size)]
        return lax.dot_general(
            fbuf[slot], expand_bits(packed), (((1,), (0,)), ((), ())), preferred_element_type=jnp.float32
        )

    early = n_col - 2

    @pl.loop(0, early * halves)
    def _(t):
        step = t // halves
        start = pl.multiple_of(lax.rem(t, halves) * half, half)
        fresh = lax.rem(t, halves) == 0
        if paired:

            @pl.when(jnp.logical_and(fresh, step == 1))
            def _():
                arrived(0)

            @pl.when(jnp.logical_and(fresh, step == 2))
            def _():
                arrived(1)
                sends[3].start()
                sends[5].start()
                arrived(2)
                sends[4].start()
                sends[6].start()

            @pl.when(jnp.logical_and(fresh, step == 4))
            def _():
                arrived(5)

            @pl.when(jnp.logical_and(fresh, step == 5))
            def _():
                arrived(6)
                arrived(3)
                arrived(4)
                sends[7].start()

            slot = c
            for number, choice in enumerate((slots[0], slots[1], slots[2], slots[5], slots[6])):
                slot = jnp.where(step == number + 1, choice, slot)
        else:
            slot = lax.rem(c + n_col - step, n_col)

            @pl.when(jnp.logical_and(fresh, step > 0))
            def _():
                send(fbuf.at[slot], fbuf.at[slot], step - 1, mates[0]).wait_recv()

        total[:, pl.ds(start, half)] += product(slot, start, half)

    if paired:
        arrived(7)
        last = (slots[3], slots[7])
    else:
        last = (lax.rem(c + 2, n_col), lax.rem(c + 1, n_col))
        for slot, role in zip(last, (n_col - 3, n_col - 2)):
            send(fbuf.at[slot], fbuf.at[slot], role, mates[0]).wait_recv()

    def exchange(t, other):
        return pltpu.make_async_remote_copy(
            src_ref=out_code.at[t], dst_ref=in_code.at[t], send_sem=psend.at[t], recv_sem=precv.at[t],
            device_id={"row": other}, device_id_type=MESH,
        )

    @pl.loop(0, n_row)
    def _(t):
        other = lax.rem(r + 1 + t, n_row)
        start = pl.multiple_of(other * part, part)
        block = total[:, pl.ds(start, part)] + product(last[0], start, part)
        block = block + product(last[1], start, part)

        @pl.when(t < n_row - 1)
        def _():
            out_code[t] = encode(block, scale)
            exchange(t, other).start()

        @pl.when(t == n_row - 1)
        def _():
            total[:, pl.ds(0, part)] = block

    def received(t, value):
        exchange(t, others[0]).wait_recv()
        return value + decode(in_code[t], scale)

    reached = total[:, pl.ds(0, part)]
    for t in range(n_row - 1):
        reached = received(t, reached)
    place = lax.broadcasted_iota(jnp.int32, (32, part), 0)
    kept, added = [], []
    for word in range(visited.shape[0]):
        value = reached[word * 32 : word * 32 + 32]
        unseen = ((visited[word : word + 1, :] >> place) & 1) == 0
        kept.append(jnp.where(unseen, value, 0.0))
        marks = jnp.where(jnp.logical_and(unseen, value > 0), jnp.int32(1) << place, 0)
        added.append(jnp.sum(marks, axis=0, keepdims=True))
    counts[...] = jnp.concatenate(kept, axis=0).T
    bits[...] = visited[...] | jnp.concatenate(added, axis=0)
    for copy in sends:
        copy.wait_send()
    for t in range(n_row - 1):
        exchange(t, others[0]).wait_send()


def span(c):
    return flip(c, 1), flip(c, 2), flip(c, 4)


def unpack(packed):
    one = jnp.full((32, packed.shape[1]), 1, jnp.float8_e4m3fn)
    zero = jnp.full((32, packed.shape[1]), 0, jnp.float8_e4m3fn)
    pieces = []
    for block in range(packed.shape[0] // 32):
        part = packed[block * 32 : block * 32 + 32]
        for bit in range(8):
            mask = np.int8(-128) if bit == 7 else np.int8(1 << bit)
            pieces.append(jnp.where((part & mask) != 0, one, zero))
    return jnp.concatenate(pieces, axis=0)


def grouped(n_group, adj, src, vis, counts, bits, stage, bytes_, own_f, own_v, own_sum, *rest):
    fb, rem, out_code, in_code = (rest[i * n_group : i * n_group + n_group] for i in range(4))
    load_sem, own_sem, fsend, frecv, psend, precv = rest[4 * n_group :]
    n_row, n_col = 4, 8
    r, c = lax.axis_index("row"), lax.axis_index("col")
    dst, width = adj.shape
    depth, roots = src.shape
    part = dst // n_row
    wide = width // n_col * 4
    tile = stage.shape[1]
    tiles = dst // tile
    depth2 = depth // 2
    scale = LEVELS / math.log(width * 64 * 1.01 / LOW)
    pair, east, north = span(c)
    diagonal = flip(east, 4)
    slots = [c, pair, east, north, flip(pair, 2), flip(pair, 4), diagonal, flip(diagonal, 1)]
    middle = jnp.logical_or(r == 1, r == 2)
    high = r // 2
    edge_order, middle_order = (3, 2, 1), (2, 3, 0)
    order = []
    for a, b in zip(edge_order, middle_order):
        low = jnp.where(middle, b, a)
        order.append(low + high * (3 - 2 * low))
    relay = 1 + high

    barrier = pltpu.get_barrier_semaphore()
    for mate in (pair, east, north):
        pl.semaphore_signal(barrier, inc=1, device_id={"col": mate}, device_id_type=MESH)
    for i in range(1, n_row):
        pl.semaphore_signal(barrier, inc=1, device_id={"row": lax.rem(r + i, n_row)}, device_id_type=MESH)

    frontier_copy = pltpu.make_async_copy(src, own_f, own_sem.at[0])
    frontier_copy.start()
    visited_copy = pltpu.make_async_copy(vis, own_v, own_sem.at[1])
    visited_copy.start()

    def load(t, slot):
        return pltpu.make_async_copy(
            adj.at[pl.ds(pl.multiple_of(t * tile, tile), tile), :], stage.at[slot], load_sem.at[slot]
        )

    ahead = stage.shape[0] - 1
    for t in range(ahead):
        load(t, t).start()

    line = lax.broadcasted_iota(jnp.int32, (256, 256), 0)
    place = lax.broadcasted_iota(jnp.int32, (256, 256), 1)
    target = (line % 8) * 32 + ((line // 8) % 4) * 8 + line // 32
    shuffle = jnp.where(target == place, 1.0, 0.0).astype(jnp.bfloat16)
    frontier_copy.wait()
    for block in range(depth // 256):
        moved = lax.dot_general(
            own_f[block * 256 : block * 256 + 256, :], shuffle, (((0,), (0,)), ((), ())),
            preferred_element_type=jnp.float32,
        ).astype(jnp.bfloat16)
        first = 0
        for g in range(n_group):
            rows = fb[g].shape[1]
            fb[g][c, :, block * 256 : block * 256 + 256] = moved[first : first + rows]
            first += rows

    def half(g, slot, h):
        return fb[g].at[slot, :, pl.ds(h * depth2, depth2)]

    def send(ref, g, role, h, mate):
        return pltpu.make_async_remote_copy(
            src_ref=ref, dst_ref=ref, send_sem=fsend.at[g, role, h], recv_sem=frecv.at[g, role, h],
            device_id={"col": mate}, device_id_type=MESH,
        )

    def to_pair(g):
        return send(fb[g].at[c], g, 0, 0, pair)

    def message(g, role, h):
        source, mate = {
            1: (c, east), 2: (c, north), 3: (east, north), 4: (north, east),
            5: (east, pair), 6: (north, pair), 7: (diagonal, pair),
        }[role]
        return send(half(g, source, h), g, role, h, mate)

    def arrived(g, role, h):
        slot = {1: east, 2: north, 3: diagonal, 4: diagonal, 5: slots[4], 6: slots[5], 7: slots[7]}[role]
        send(half(g, slot, h), g, role, h, pair).wait_recv()

    def first_sends(g):
        message(g, 1, 0).start()
        message(g, 2, 1).start()
        message(g, 1, 1).start()
        message(g, 2, 0).start()

    pl.semaphore_wait(barrier, 6)
    first_sends(0)
    for g in range(n_group):
        to_pair(g).start()

    @pl.loop(0, tiles)
    def _(t):
        slot = lax.rem(t, ahead + 1)

        @pl.when(t + ahead < tiles)
        def _():
            load(t + ahead, lax.rem(t + ahead, ahead + 1)).start()

        load(t, slot).wait()
        turned = stage[slot].T.reshape(width // 8, 8, tile)
        spread = jnp.concatenate([turned, turned >> 8, turned >> 16, turned >> 24], axis=1)
        bytes_[:, pl.ds(pl.multiple_of(t * tile, tile), tile)] = spread.reshape(width * 4, tile).astype(jnp.int8)

    def product(lhs, slot, start, size):
        packed = bytes_[pl.ds(pl.multiple_of(slot * wide, wide), wide), pl.ds(start, size)]
        return lax.dot_general(
            lhs, unpack(packed), (((1,), (0,)), ((), ())), preferred_element_type=jnp.float32
        )

    def exchange(g, t, slot, other):
        return pltpu.make_async_remote_copy(
            src_ref=out_code[g].at[t], dst_ref=in_code[g].at[slot], send_sem=psend.at[g, t],
            recv_sem=precv.at[g, slot], device_id={"row": other}, device_id_type=MESH,
        )

    def received(g, slot):
        exchange(g, 0, slot, relay).wait_recv()
        return decode(in_code[g][slot], scale)

    def pass_on(g):
        @pl.when(middle)
        def _():
            out_code[g][1] = encode(rem[g][1] + received(g, n_row), scale)
            exchange(g, 1, r, order[1]).start()

    for g in range(n_group):
        rem[g][...] = jnp.zeros_like(rem[g])
        arrived(g, 1, 0)
        message(g, 3, 0).start()
        arrived(g, 2, 1)
        message(g, 4, 1).start()
        if g + 1 < n_group:
            first_sends(g + 1)
        message(g, 5, 0).start()
        message(g, 6, 1).start()

        @pl.loop(0, 6)
        def _(step):
            @pl.when(step == 1)
            def _():
                send(fb[g].at[pair], g, 0, 0, pair).wait_recv()

            @pl.when(step == 2)
            def _():
                arrived(g, 1, 1)
                message(g, 5, 1).start()
                arrived(g, 2, 0)
                message(g, 6, 0).start()

            if g:
                @pl.when(step == 3)
                def _():
                    pass_on(g - 1)

            @pl.when(step == 4)
            def _():
                arrived(g, 5, 0)
                arrived(g, 5, 1)

            @pl.when(step == 5)
            def _():
                arrived(g, 6, 0)
                arrived(g, 6, 1)
                arrived(g, 3, 0)
                message(g, 7, 0).start()
                arrived(g, 4, 1)
                message(g, 7, 1).start()

            slot = slots[0]
            for number in range(1, 6):
                slot = jnp.where(step == number, slots[number], slot)
            lhs = fb[g][slot]
            for t in range(3):
                rem[g][t] += product(lhs, slot, pl.multiple_of(order[t] * part, part), part)

        arrived(g, 7, 0)
        arrived(g, 7, 1)

        @pl.loop(0, 3)
        def _(t):
            target = jnp.where(t == 0, order[0], jnp.where(t == 1, order[1], order[2]))
            start = pl.multiple_of(target * part, part)
            value = rem[g][t] + product(fb[g][slots[6]], slots[6], start, part)
            value = value + product(fb[g][slots[7]], slots[7], start, part)
            direct = jnp.logical_or(t != 1, jnp.logical_not(middle))

            @pl.when(direct)
            def _():
                out_code[g][t] = encode(value, scale)
                first_edge = jnp.logical_and(t == 0, jnp.logical_not(middle))
                exchange(g, t, jnp.where(first_edge, n_row, r), jnp.where(first_edge, relay, target)).start()

            @pl.when(jnp.logical_not(direct))
            def _():
                rem[g][t] = value

    quarter = part // 4

    @pl.loop(0, 4)
    def _(q):
        @pl.when(q == 3)
        def _():
            pass_on(n_group - 1)

        start = pl.multiple_of(r * part + q * quarter, quarter)
        value = jnp.zeros((roots, quarter), jnp.float32)
        for slot in slots:
            lhs = jnp.concatenate([ref[slot] for ref in fb], axis=0)
            value = value + product(lhs, slot, start, quarter)
        own_sum[:, pl.ds(pl.multiple_of(q * quarter, quarter), quarter)] = value

    senders = [
        jnp.where(middle, 2 - high, 1 + high),
        jnp.where(middle, 3 - 3 * high, 2 - high),
    ]
    first = 0
    for g in range(n_group):
        rows = fb[g].shape[1]

        for sender in senders:
            own_sum[pl.ds(first, rows), :] += received(g, sender)

        @pl.when(middle)
        def _():
            own_sum[pl.ds(first, rows), :] += received(g, 3 * high)

        first += rows

    visited_copy.wait()
    reached = own_sum[...]
    place = lax.broadcasted_iota(jnp.int32, (32, part), 0)
    kept, added = [], []
    for word in range(own_v.shape[0]):
        value = reached[word * 32 : word * 32 + 32]
        unseen = ((own_v[word : word + 1, :] >> place) & 1) == 0
        kept.append(jnp.where(unseen, value, 0.0))
        marks = jnp.where(jnp.logical_and(unseen, value > 0), jnp.int32(1) << place, 0)
        added.append(jnp.sum(marks, axis=0, keepdims=True))
    counts[...] = jnp.concatenate(kept, axis=0).T
    bits[...] = own_v[...] | jnp.concatenate(added, axis=0)

    for g in range(n_group):
        to_pair(g).wait_send()
        for role, h in ((1, 0), (1, 1), (2, 0), (2, 1), (3, 0), (4, 1), (5, 0), (5, 1), (6, 0), (6, 1), (7, 0), (7, 1)):
            message(g, role, h).wait_send()
        for t in range(3):
            exchange(g, t, r, relay).wait_send()


def grouped_shards(adjacency, frontier, visited):
    dst, width = adjacency.shape
    depth, roots = frontier.shape
    part = dst // 4
    tile = math.gcd(dst, 512)
    groups = (roots // 2, roots // 2)
    n_group = len(groups)
    anywhere = pl.BlockSpec(memory_space=pl.ANY)
    vmem = pl.BlockSpec(memory_space=pltpu.VMEM)
    dma = pltpu.SemaphoreType.DMA
    return pl.pallas_call(
        functools.partial(grouped, n_group),
        out_shape=(
            jax.ShapeDtypeStruct((part, roots), jnp.float32),
            jax.ShapeDtypeStruct((visited.shape[0], part), jnp.int32),
        ),
        in_specs=[anywhere] * 3,
        out_specs=(vmem, vmem),
        scratch_shapes=[
            pltpu.VMEM((4, tile, width), jnp.int32),
            pltpu.VMEM((width * 4, dst), jnp.int8),
            pltpu.VMEM((depth, roots), jnp.bfloat16),
            pltpu.VMEM(visited.shape, jnp.int32),
            pltpu.VMEM((roots, part), jnp.float32),
            *[pltpu.VMEM((8, rows, depth), jnp.bfloat16) for rows in groups],
            *[pltpu.VMEM((3, rows, part), jnp.float32) for rows in groups],
            *[pltpu.VMEM((3, rows, part), jnp.int16) for rows in groups],
            *[pltpu.VMEM((5, rows, part), jnp.int16) for rows in groups],
            dma((4,)),
            dma((2,)),
            dma((n_group, 8, 2)),
            dma((n_group, 8, 2)),
            dma((n_group, 3)),
            dma((n_group, 5)),
        ],
        compiler_params=pltpu.CompilerParams(
            collective_id=0, has_side_effects=True, vmem_limit_bytes=56 * 2**20
        ),
    )(adjacency, frontier, visited)


def shards(n_row, n_col, adjacency, frontier, visited):
    dst, width = adjacency.shape
    depth, roots = frontier.shape
    part = dst // n_row
    tile = math.gcd(dst, 256)
    ft = jnp.transpose(frontier.reshape(depth // 32, 32, roots), (2, 1, 0)).reshape(roots, depth)
    vmem = pl.BlockSpec(memory_space=pltpu.VMEM)
    roles = 8 if n_col == 8 else n_col - 1
    dma = pltpu.SemaphoreType.DMA
    return pl.pallas_call(
        functools.partial(kernel, n_row, n_col),
        out_shape=(
            jax.ShapeDtypeStruct((part, roots), jnp.float32),
            jax.ShapeDtypeStruct((visited.shape[0], part), jnp.int32),
        ),
        in_specs=[pl.BlockSpec(memory_space=pl.ANY), vmem, vmem],
        out_specs=(vmem, vmem),
        scratch_shapes=[
            pltpu.VMEM((2, tile, width), jnp.int32),
            pltpu.VMEM((width, dst), jnp.int32),
            pltpu.VMEM((n_col, roots, depth), jnp.bfloat16),
            pltpu.VMEM((roots, dst), jnp.float32),
            pltpu.VMEM((n_row - 1, roots, part), jnp.int16),
            pltpu.VMEM((n_row - 1, roots, part), jnp.int16),
            dma((2,)),
            dma,
            dma((roles,)),
            dma((roles,)),
            dma((n_row - 1,)),
            dma((n_row - 1,)),
        ],
        compiler_params=pltpu.CompilerParams(
            collective_id=0, has_side_effects=True, vmem_limit_bytes=56 * 2**20
        ),
    )(adjacency, ft, visited)


def solution(mesh):
    placed = (P("col", "row"), P(("row", "col"), None), P(None, ("col", "row")))
    n_row, n_col = mesh.shape["row"], mesh.shape["col"]
    body = grouped_shards if (n_row, n_col) == (4, 8) else functools.partial(shards, n_row, n_col)
    return jax.shard_map(
        body,
        mesh=mesh,
        in_specs=placed,
        out_specs=(P(("col", "row"), None), P(None, ("col", "row"))),
        check_vma=False,
    )
```

```python
import functools
import math

import jax
import jax.numpy as jnp
import numpy as np
from jax import lax
from jax.experimental import pallas as pl
from jax.experimental.pallas import tpu as pltpu
from jax.sharding import PartitionSpec as P

MESH = pl.DeviceIdType.MESH
LOW = 0.09
LEVELS = 65000.0


def expand_bits(words):
    one = jnp.full(words.shape, 1, jnp.float8_e4m3fn)
    zero = jnp.full(words.shape, 0, jnp.float8_e4m3fn)
    pieces = []
    for byte in range(4):
        part = (words >> (8 * byte)).astype(jnp.int8)
        for bit in range(8):
            mask = np.int8(-128) if bit == 7 else np.int8(1 << bit)
            pieces.append(jnp.where((part & mask) != 0, one, zero))
    return jnp.concatenate(pieces, axis=0)


def encode(value, scale):
    code = jnp.log(jnp.maximum(value, LOW)) * scale + (1.5 - math.log(LOW) * scale)
    code = jnp.where(value > 0, code, 0.0).astype(jnp.int32)
    return (code - 32768).astype(jnp.int16)


def decode(code, scale):
    code = code.astype(jnp.int32) + 32768
    value = jnp.exp((code - 1).astype(jnp.float32) * (1.0 / scale) + math.log(LOW))
    return jnp.where(code > 0, value, 0.0)


def flip(index, bit):
    return index + bit - 2 * bit * ((index // bit) % 2)


def kernel(
    n_row, n_col, adj, ft, visited, counts, bits,
    stage, words, fbuf, total, out_code, in_code,
    load_sem, own_sem, fsend, frecv, psend, precv,
):
    r, c = lax.axis_index("row"), lax.axis_index("col")
    dst, width = adj.shape
    depth = ft.shape[1]
    wide = width // n_col
    part = dst // n_row
    half = math.gcd(dst, 2048)
    halves = dst // half
    tile = stage.shape[1]
    tiles = dst // tile
    paired = n_col == 8
    scale = LEVELS / math.log(width * 32 * 1.01 / LOW)

    def load(t, slot):
        return pltpu.make_async_copy(
            adj.at[pl.ds(pl.multiple_of(t * tile, tile), tile), :], stage.at[slot], load_sem.at[slot]
        )

    load(0, 0).start()
    own = pltpu.make_async_copy(ft, fbuf.at[c], own_sem)
    own.start()

    if paired:
        mates = [flip(c, 1), flip(c, 2), flip(c, 4)]
    else:
        mates = [lax.rem(c + i, n_col) for i in range(1, n_col)]
    others = [lax.rem(r + i, n_row) for i in range(1, n_row)]
    barrier = pltpu.get_barrier_semaphore()
    for mate in mates:
        pl.semaphore_signal(barrier, inc=1, device_id={"col": mate}, device_id_type=MESH)
    for other in others:
        pl.semaphore_signal(barrier, inc=1, device_id={"row": other}, device_id_type=MESH)
    pl.semaphore_wait(barrier, len(mates) + len(others))

    def send(src, dst_ref, role, mate):
        return pltpu.make_async_remote_copy(
            src_ref=src, dst_ref=dst_ref, send_sem=fsend.at[role], recv_sem=frecv.at[role],
            device_id={"col": mate}, device_id_type=MESH,
        )

    if paired:
        pair, east, north = mates
        first, second = pl.ds(0, ft.shape[0] // 2), pl.ds(ft.shape[0] // 2, ft.shape[0] // 2)
        diagonal = flip(east, 4)
        slots = [pair, east, north, diagonal, diagonal, flip(pair, 2), flip(pair, 4), flip(diagonal, 1)]
        sends = [
            send(ft, fbuf.at[c], 0, pair),
            send(ft, fbuf.at[c], 1, east),
            send(ft, fbuf.at[c], 2, north),
            send(fbuf.at[east, first], fbuf.at[east, first], 3, north),
            send(fbuf.at[north, second], fbuf.at[north, second], 4, east),
            send(fbuf.at[east], fbuf.at[east], 5, pair),
            send(fbuf.at[north], fbuf.at[north], 6, pair),
            send(fbuf.at[diagonal], fbuf.at[diagonal], 7, pair),
        ]
        for role in (1, 2, 0):
            sends[role].start()

        def arrived(role):
            place = fbuf.at[slots[role]]
            if role == 3:
                place = fbuf.at[diagonal, first]
            if role == 4:
                place = fbuf.at[diagonal, second]
            send(place, place, role, pair).wait_recv()

    else:
        sends = [send(ft, fbuf.at[c], i, mate) for i, mate in enumerate(mates)]
        for copy in sends:
            copy.start()

    @pl.loop(0, tiles)
    def _(t):
        slot = lax.rem(t, 2)

        @pl.when(t + 1 < tiles)
        def _():
            load(t + 1, 1 - slot).start()

        load(t, slot).wait()
        words[:, pl.ds(pl.multiple_of(t * tile, tile), tile)] = stage[slot].T

    total[...] = jnp.zeros_like(total)
    own.wait()

    def product(slot, start, size):
        packed = words[pl.ds(pl.multiple_of(slot * wide, wide), wide), pl.ds(start, size)]
        return lax.dot_general(
            fbuf[slot], expand_bits(packed), (((1,), (0,)), ((), ())), preferred_element_type=jnp.float32
        )

    early = n_col - 2

    @pl.loop(0, early * halves)
    def _(t):
        step = t // halves
        start = pl.multiple_of(lax.rem(t, halves) * half, half)
        fresh = lax.rem(t, halves) == 0
        if paired:

            @pl.when(jnp.logical_and(fresh, step == 1))
            def _():
                arrived(0)

            @pl.when(jnp.logical_and(fresh, step == 2))
            def _():
                arrived(1)
                sends[3].start()
                sends[5].start()
                arrived(2)
                sends[4].start()
                sends[6].start()

            @pl.when(jnp.logical_and(fresh, step == 4))
            def _():
                arrived(5)

            @pl.when(jnp.logical_and(fresh, step == 5))
            def _():
                arrived(6)
                arrived(3)
                arrived(4)
                sends[7].start()

            slot = c
            for number, choice in enumerate((slots[0], slots[1], slots[2], slots[5], slots[6])):
                slot = jnp.where(step == number + 1, choice, slot)
        else:
            slot = lax.rem(c + n_col - step, n_col)

            @pl.when(jnp.logical_and(fresh, step > 0))
            def _():
                send(fbuf.at[slot], fbuf.at[slot], step - 1, mates[0]).wait_recv()

        total[:, pl.ds(start, half)] += product(slot, start, half)

    if paired:
        arrived(7)
        last = (slots[3], slots[7])
    else:
        last = (lax.rem(c + 2, n_col), lax.rem(c + 1, n_col))
        for slot, role in zip(last, (n_col - 3, n_col - 2)):
            send(fbuf.at[slot], fbuf.at[slot], role, mates[0]).wait_recv()

    def exchange(t, other):
        return pltpu.make_async_remote_copy(
            src_ref=out_code.at[t], dst_ref=in_code.at[t], send_sem=psend.at[t], recv_sem=precv.at[t],
            device_id={"row": other}, device_id_type=MESH,
        )

    @pl.loop(0, n_row)
    def _(t):
        other = lax.rem(r + 1 + t, n_row)
        start = pl.multiple_of(other * part, part)
        block = total[:, pl.ds(start, part)] + product(last[0], start, part)
        block = block + product(last[1], start, part)

        @pl.when(t < n_row - 1)
        def _():
            out_code[t] = encode(block, scale)
            exchange(t, other).start()

        @pl.when(t == n_row - 1)
        def _():
            total[:, pl.ds(0, part)] = block

    def received(t, value):
        exchange(t, others[0]).wait_recv()
        return value + decode(in_code[t], scale)

    reached = total[:, pl.ds(0, part)]
    for t in range(n_row - 1):
        reached = received(t, reached)
    place = lax.broadcasted_iota(jnp.int32, (32, part), 0)
    kept, added = [], []
    for word in range(visited.shape[0]):
        value = reached[word * 32 : word * 32 + 32]
        unseen = ((visited[word : word + 1, :] >> place) & 1) == 0
        kept.append(jnp.where(unseen, value, 0.0))
        marks = jnp.where(jnp.logical_and(unseen, value > 0), jnp.int32(1) << place, 0)
        added.append(jnp.sum(marks, axis=0, keepdims=True))
    counts[...] = jnp.concatenate(kept, axis=0).T
    bits[...] = visited[...] | jnp.concatenate(added, axis=0)
    for copy in sends:
        copy.wait_send()
    for t in range(n_row - 1):
        exchange(t, others[0]).wait_send()


ROLES = 19


def unpack(packed):
    one = jnp.full((32, packed.shape[1]), 1, jnp.float8_e4m3fn)
    zero = jnp.full((32, packed.shape[1]), 0, jnp.float8_e4m3fn)
    pieces = []
    for block in range(packed.shape[0] // 32):
        part = packed[block * 32 : block * 32 + 32]
        for bit in range(8):
            mask = np.int8(-128) if bit == 7 else np.int8(1 << bit)
            pieces.append(jnp.where((part & mask) != 0, one, zero))
    return jnp.concatenate(pieces, axis=0)


def grouped(
    groups, adj, src, own_sum,
    stage, packed, own_f, fb, rem, out_code, in_code,
    load_sem, own_sem, fsend, frecv, psend, precv,
):
    n_row, n_col = 4, 8
    r, c = lax.axis_index("row"), lax.axis_index("col")
    dst, width = adj.shape
    depth, roots = src.shape
    part = dst // n_row
    wide = width // n_col * 4
    lanes = width // 4
    tile = dst // 2
    scale = LEVELS / math.log(width * 64 * 1.01 / LOW)
    last = len(groups) - 1
    firsts = [sum(groups[:g]) for g in range(len(groups))]
    pair, east, north = flip(c, 1), flip(c, 2), flip(c, 4)
    diagonal = flip(east, 4)
    slots = [c, pair, east, north, flip(pair, 2), flip(pair, 4), diagonal, flip(diagonal, 1)]
    blocks = [0, 0, 1, 2, 1, 2, 3, 3]
    middle = jnp.logical_or(r == 1, r == 2)
    high = r // 2
    relay = 1 + high
    order = []
    for a, b in zip((3, 2, 1), (2, 3, 0)):
        low = jnp.where(middle, b, a)
        order.append(low + high * (3 - 2 * low))
    senders = [
        jnp.where(middle, 2 - high, 1 + high),
        jnp.where(middle, 3 - 3 * high, 2 - high),
    ]

    def chosen(step, values):
        value = values[0]
        for number in range(1, len(values)):
            value = jnp.where(step == number, values[number], value)
        return value

    barrier = pltpu.get_barrier_semaphore()
    for mate in (pair, east, north):
        pl.semaphore_signal(barrier, inc=1, device_id={"col": mate}, device_id_type=MESH)
    for other in senders:
        pl.semaphore_signal(barrier, inc=1, device_id={"row": other}, device_id_type=MESH)

    @pl.when(middle)
    def _():
        pl.semaphore_signal(barrier, inc=1, device_id={"row": 3 * high}, device_id_type=MESH)

    frontier_copy = pltpu.make_async_copy(src, own_f, own_sem)
    frontier_copy.start()

    def load(b, i):
        lane = pl.multiple_of(chosen(b, [slots[k] // 2 * lanes for k in (0, 2, 3, 6)]), lanes)
        lines = pl.ds(pl.multiple_of(i * tile, tile), tile)
        return pltpu.make_async_copy(
            adj.at[lines, pl.ds(lane, lanes)], stage.at[b, lines], load_sem.at[b, i]
        )

    for b in (0, 1):
        load(b, 0).start()
        load(b, 1).start()

    line = lax.broadcasted_iota(jnp.int32, (256, 256), 0)
    place = lax.broadcasted_iota(jnp.int32, (256, 256), 1)
    target = (line % 8) * 32 + ((line // 8) % 4) * 8 + line // 32
    shuffle = jnp.where(target == place, 1.0, 0.0).astype(jnp.bfloat16)
    frontier_copy.wait()
    for block in range(depth // 256):
        columns = slice(block * 256, block * 256 + 256)
        fb[c, :, columns] = lax.dot_general(
            own_f[columns, :], shuffle, (((0,), (0,)), ((), ())), preferred_element_type=jnp.float32
        ).astype(jnp.bfloat16)

    def rows(g):
        return pl.ds(firsts[g], groups[g])

    def send(ref, g, role, i, mate):
        number = g * ROLES + (0, 1, 5, 9, 9, 13, 15, 17)[role] + i
        return pltpu.make_async_remote_copy(
            src_ref=ref, dst_ref=ref, send_sem=fsend.at[number], recv_sem=frecv.at[number],
            device_id={"col": mate}, device_id_type=MESH,
        )

    def piece(g, role, i, slot):
        size = depth // 4 if role < 5 else depth // 2
        return fb.at[slot, rows(g), pl.ds(i * size, size)]

    def to_pair(g):
        return send(fb.at[c, rows(g)], g, 0, 0, pair)

    def message(g, role, i):
        source, mate = {
            1: (c, east), 2: (c, north), 3: (east, north), 4: (north, east),
            5: (east, pair), 6: (north, pair), 7: (diagonal, pair),
        }[role]
        return send(piece(g, role, i, source), g, role, i, mate)

    def arrived(g, role, i):
        slot = {1: 2, 2: 3, 3: 6, 4: 6, 5: 4, 6: 5, 7: 7}[role]
        send(piece(g, role, i, slots[slot]), g, role, i, pair).wait_recv()

    def first_sends(g):
        for i in range(4):
            message(g, 1, i).start()
            message(g, 2, (i + 2) % 4).start()

    def forward(g, i):
        arrived(g, 1, i)
        message(g, 3, i).start()
        arrived(g, 2, i + 2)
        message(g, 4, i + 2).start()

    def forward_rest(g):
        forward(g, 1)
        if g < last:
            first_sends(g + 1)
        message(g, 5, 0).start()
        message(g, 6, 1).start()

    def share_rest(g):
        arrived(g, 1, 2)
        arrived(g, 1, 3)
        message(g, 5, 1).start()
        arrived(g, 2, 0)
        arrived(g, 2, 1)
        message(g, 6, 0).start()

    def share_diagonal(g):
        arrived(g, 3, 0)
        arrived(g, 3, 1)
        message(g, 7, 0).start()
        arrived(g, 4, 2)
        arrived(g, 4, 3)
        message(g, 7, 1).start()

    pl.semaphore_wait(barrier, 5 + jnp.where(middle, 1, 0))
    first_sends(0)
    for g in range(len(groups)):
        to_pair(g).start()
    for b in (2, 3):
        load(b, 0).start()
        load(b, 1).start()

    def turn(b, i):
        load(b, i).wait()
        columns = pl.ds(pl.multiple_of(i * tile, tile), tile)
        turned = stage[b, columns, :].T.reshape(lanes // 8, 8, tile)
        spread = jnp.concatenate([turned, turned >> 8, turned >> 16, turned >> 24], axis=1)
        target = pl.ds(pl.multiple_of(b * lanes * 4, lanes * 4), lanes * 4)
        packed[target, columns] = spread.reshape(lanes * 4, tile).astype(jnp.int8)

    def product(lhs, slot, block, start, size):
        base = pl.multiple_of(block * lanes * 4 + lax.rem(slot, 2) * wide, wide)
        return lax.dot_general(
            lhs, unpack(packed[pl.ds(base, wide), pl.ds(start, size)]), (((1,), (0,)), ((), ())),
            preferred_element_type=jnp.float32,
        )

    def add_step(span, pairs):
        for t in range(3):
            start = pl.multiple_of(order[t] * part, part)
            value = rem[t, span, :]
            for slot, block in pairs:
                value = value + product(fb[slot, span, :], slot, block, start, part)
            rem[t, span, :] = value

    def exchange(g, t, slot, other):
        return pltpu.make_async_remote_copy(
            src_ref=out_code.at[t, rows(g)], dst_ref=in_code.at[slot, rows(g)], send_sem=psend.at[g, t],
            recv_sem=precv.at[g, slot], device_id={"row": other}, device_id_type=MESH,
        )

    def received(g, slot):
        exchange(g, 0, slot, relay).wait_recv()
        return decode(in_code[slot, rows(g), :], scale)

    def pass_on(g):
        @pl.when(middle)
        def _():
            out_code[1, rows(g), :] = encode(rem[1, rows(g), :] + received(g, n_row), scale)
            exchange(g, 1, r, order[1]).start()

    rem[...] = jnp.zeros_like(rem)

    @pl.loop(0, 2)
    def _(i):
        turn(0, i)

    @pl.loop(0, 2)
    def _(step):
        @pl.when(step == 1)
        def _():
            forward(0, 0)
            for g in range(len(groups)):
                send(fb.at[pair, rows(g)], g, 0, 0, pair).wait_recv()

        add_step(pl.ds(0, roots), [(chosen(step, (c, pair)), 0)])
        for k in range(3):
            number = step * 3 + k
            turn(1 + number // 2, lax.rem(number, 2))

    forward_rest(0)

    for g in range(len(groups)):
        share_rest(g)

        @pl.loop(0, 2)
        def _(step):
            @pl.when(step == 1)
            def _():
                share_diagonal(g)
                if 0 < g < last:
                    forward(g + 1, 0)
                for i in (0, 1):
                    arrived(g, 5, i)
                    arrived(g, 6, i)

            add_step(rows(g), [(chosen(step, slots[k : k + 3 : 2]), k - 1) for k in (2, 3)])

        if g == 0 < last:
            forward(1, 0)
        if g:
            pass_on(g - 1)
        if g < last:
            forward_rest(g + 1)
        arrived(g, 7, 0)
        arrived(g, 7, 1)

        @pl.loop(0, 3)
        def _(t):
            target = chosen(t, order)
            start = pl.multiple_of(target * part, part)
            value = rem[t, rows(g), :]
            for slot in slots[6:]:
                value = value + product(fb[slot, rows(g), :], slot, 3, start, part)
            direct = jnp.logical_or(t != 1, jnp.logical_not(middle))

            @pl.when(direct)
            def _():
                out_code[t, rows(g), :] = encode(value, scale)
                first_edge = jnp.logical_and(t == 0, jnp.logical_not(middle))
                exchange(g, t, jnp.where(first_edge, n_row, r), jnp.where(first_edge, relay, target)).start()

            @pl.when(jnp.logical_not(direct))
            def _():
                rem[t, rows(g), :] = value

    quarter = part // 4

    @pl.loop(0, 4)
    def _(q):
        @pl.when(q == 2)
        def _():
            pass_on(last)

        start = pl.multiple_of(r * part + q * quarter, quarter)
        value = jnp.zeros((roots, quarter), jnp.float32)
        for slot, block in zip(slots, blocks):
            value = value + product(fb[slot], slot, block, start, quarter)
        own_sum[:, pl.ds(pl.multiple_of(q * quarter, quarter), quarter)] = value

    for g in range(len(groups)):
        to_pair(g).wait_send()
        for role, places in ((1, 4), (2, 4), (3, 2), (4, 2), (5, 2), (6, 2), (7, 2)):
            for i in range(places):
                message(g, role, i + 2 if role == 4 else i).wait_send()
    for g in range(last):
        for t in range(3):
            exchange(g, t, r, relay).wait_send()
    for g in range(len(groups)):
        for sender in senders:
            own_sum[rows(g), :] += received(g, sender)

        @pl.when(middle)
        def _():
            own_sum[rows(g), :] += received(g, 3 * high)

    for t in range(3):
        exchange(last, t, r, relay).wait_send()


def deliver(reached, visited, counts, bits, held, marked, sem):
    part, roots = held.shape
    size = part // 4

    def copy(i):
        span = pl.ds(i * size, size)
        return pltpu.make_async_copy(held.at[span, :], counts.at[span, :], sem.at[i])

    place = lax.broadcasted_iota(jnp.int32, (32, size), 0)
    for i in range(4):
        span = slice(i * size, i * size + size)
        kept, added = [], []
        for word in range(visited.shape[0]):
            value = reached[word * 32 : word * 32 + 32, span]
            unseen = ((visited[word : word + 1, span] >> place) & 1) == 0
            kept.append(jnp.where(unseen, value, 0.0))
            marks = jnp.where(jnp.logical_and(unseen, value > 0), jnp.int32(1) << place, 0)
            added.append(jnp.sum(marks, axis=0, keepdims=True))
        held[span, :] = jnp.concatenate(kept, axis=0).T
        marked[:, span] = visited[:, span] | jnp.concatenate(added, axis=0)
        if i:
            copy(i - 1).start()
    last = pltpu.make_async_copy(marked, bits, sem.at[4])
    copy(3).start()
    last.start()
    for i in range(4):
        copy(i).wait()
    last.wait()


def grouped_shards(adjacency, frontier, visited):
    dst, width = adjacency.shape
    depth, roots = frontier.shape
    part = dst // 4
    groups = (roots // 2, roots // 2)
    n_group = len(groups)
    anywhere = pl.BlockSpec(memory_space=pl.ANY)
    vmem = pl.BlockSpec(memory_space=pltpu.VMEM)
    dma = pltpu.SemaphoreType.DMA
    reached = pl.pallas_call(
        functools.partial(grouped, groups),
        out_shape=jax.ShapeDtypeStruct((roots, part), jnp.float32),
        in_specs=[anywhere] * 2,
        out_specs=vmem,
        scratch_shapes=[
            pltpu.VMEM((4, dst, width // 4), jnp.int32),
            pltpu.VMEM((width * 4, dst), jnp.int8),
            pltpu.VMEM((depth, roots), jnp.bfloat16),
            pltpu.VMEM((8, roots, depth), jnp.bfloat16),
            pltpu.VMEM((3, roots, part), jnp.float32),
            pltpu.VMEM((3, roots, part), jnp.int16),
            pltpu.VMEM((5, roots, part), jnp.int16),
            dma((4, 2)),
            dma,
            dma((n_group * ROLES,)),
            dma((n_group * ROLES,)),
            dma((n_group, 3)),
            dma((n_group, 5)),
        ],
        compiler_params=pltpu.CompilerParams(
            collective_id=0, has_side_effects=True, vmem_limit_bytes=53 * 2**20
        ),
    )(adjacency, frontier)
    return pl.pallas_call(
        deliver,
        out_shape=(
            jax.ShapeDtypeStruct((part, roots), jnp.float32),
            jax.ShapeDtypeStruct((visited.shape[0], part), jnp.int32),
        ),
        in_specs=[vmem] * 2,
        out_specs=(anywhere, anywhere),
        scratch_shapes=[
            pltpu.VMEM((part, roots), jnp.float32),
            pltpu.VMEM((visited.shape[0], part), jnp.int32),
            dma((5,)),
        ],
        compiler_params=pltpu.CompilerParams(vmem_limit_bytes=4 * 2**20),
    )(reached, visited)


def shards(n_row, n_col, adjacency, frontier, visited):
    dst, width = adjacency.shape
    depth, roots = frontier.shape
    part = dst // n_row
    tile = math.gcd(dst, 256)
    ft = jnp.transpose(frontier.reshape(depth // 32, 32, roots), (2, 1, 0)).reshape(roots, depth)
    vmem = pl.BlockSpec(memory_space=pltpu.VMEM)
    roles = 8 if n_col == 8 else n_col - 1
    dma = pltpu.SemaphoreType.DMA
    return pl.pallas_call(
        functools.partial(kernel, n_row, n_col),
        out_shape=(
            jax.ShapeDtypeStruct((part, roots), jnp.float32),
            jax.ShapeDtypeStruct((visited.shape[0], part), jnp.int32),
        ),
        in_specs=[pl.BlockSpec(memory_space=pl.ANY), vmem, vmem],
        out_specs=(vmem, vmem),
        scratch_shapes=[
            pltpu.VMEM((2, tile, width), jnp.int32),
            pltpu.VMEM((width, dst), jnp.int32),
            pltpu.VMEM((n_col, roots, depth), jnp.bfloat16),
            pltpu.VMEM((roots, dst), jnp.float32),
            pltpu.VMEM((n_row - 1, roots, part), jnp.int16),
            pltpu.VMEM((n_row - 1, roots, part), jnp.int16),
            dma((2,)),
            dma,
            dma((roles,)),
            dma((roles,)),
            dma((n_row - 1,)),
            dma((n_row - 1,)),
        ],
        compiler_params=pltpu.CompilerParams(
            collective_id=0, has_side_effects=True, vmem_limit_bytes=56 * 2**20
        ),
    )(adjacency, ft, visited)


def solution(mesh):
    placed = (P("col", "row"), P(("row", "col"), None), P(None, ("col", "row")))
    n_row, n_col = mesh.shape["row"], mesh.shape["col"]
    body = grouped_shards if (n_row, n_col) == (4, 8) else functools.partial(shards, n_row, n_col)
    return jax.shard_map(
        body,
        mesh=mesh,
        in_specs=placed,
        out_specs=(P(("col", "row"), None), P(None, ("col", "row"))),
        check_vma=False,
    )
```

```python
import functools
import math

import jax
import jax.numpy as jnp
import numpy as np
from jax import lax
from jax.experimental import pallas as pl
from jax.experimental.pallas import tpu as pltpu
from jax.sharding import PartitionSpec as P

MESH = pl.DeviceIdType.MESH
LOW = 0.09
LEVELS = 65000.0


def expand_bits(words):
    one = jnp.full(words.shape, 1, jnp.float8_e4m3fn)
    zero = jnp.full(words.shape, 0, jnp.float8_e4m3fn)
    pieces = []
    for byte in range(4):
        part = (words >> (8 * byte)).astype(jnp.int8)
        for bit in range(8):
            mask = np.int8(-128) if bit == 7 else np.int8(1 << bit)
            pieces.append(jnp.where((part & mask) != 0, one, zero))
    return jnp.concatenate(pieces, axis=0)


def encode(value, scale):
    code = jnp.log(jnp.maximum(value, LOW)) * scale + (1.5 - math.log(LOW) * scale)
    code = jnp.where(value > 0, code, 0.0).astype(jnp.int32)
    return (code - 32768).astype(jnp.int16)


def decode(code, scale):
    code = code.astype(jnp.int32) + 32768
    value = jnp.exp((code - 1).astype(jnp.float32) * (1.0 / scale) + math.log(LOW))
    return jnp.where(code > 0, value, 0.0)


def flip(index, bit):
    return index + bit - 2 * bit * ((index // bit) % 2)


def kernel(
    n_row, n_col, adj, ft, visited, counts, bits,
    stage, words, fbuf, total, out_code, in_code,
    load_sem, own_sem, fsend, frecv, psend, precv,
):
    r, c = lax.axis_index("row"), lax.axis_index("col")
    dst, width = adj.shape
    depth = ft.shape[1]
    wide = width // n_col
    part = dst // n_row
    half = math.gcd(dst, 2048)
    halves = dst // half
    tile = stage.shape[1]
    tiles = dst // tile
    paired = n_col == 8
    scale = LEVELS / math.log(width * 32 * 1.01 / LOW)

    def load(t, slot):
        return pltpu.make_async_copy(
            adj.at[pl.ds(pl.multiple_of(t * tile, tile), tile), :], stage.at[slot], load_sem.at[slot]
        )

    load(0, 0).start()
    own = pltpu.make_async_copy(ft, fbuf.at[c], own_sem)
    own.start()

    if paired:
        mates = [flip(c, 1), flip(c, 2), flip(c, 4)]
    else:
        mates = [lax.rem(c + i, n_col) for i in range(1, n_col)]
    others = [lax.rem(r + i, n_row) for i in range(1, n_row)]
    barrier = pltpu.get_barrier_semaphore()
    for mate in mates:
        pl.semaphore_signal(barrier, inc=1, device_id={"col": mate}, device_id_type=MESH)
    for other in others:
        pl.semaphore_signal(barrier, inc=1, device_id={"row": other}, device_id_type=MESH)
    pl.semaphore_wait(barrier, len(mates) + len(others))

    def send(src, dst_ref, role, mate):
        return pltpu.make_async_remote_copy(
            src_ref=src, dst_ref=dst_ref, send_sem=fsend.at[role], recv_sem=frecv.at[role],
            device_id={"col": mate}, device_id_type=MESH,
        )

    if paired:
        pair, east, north = mates
        first, second = pl.ds(0, ft.shape[0] // 2), pl.ds(ft.shape[0] // 2, ft.shape[0] // 2)
        diagonal = flip(east, 4)
        slots = [pair, east, north, diagonal, diagonal, flip(pair, 2), flip(pair, 4), flip(diagonal, 1)]
        sends = [
            send(ft, fbuf.at[c], 0, pair),
            send(ft, fbuf.at[c], 1, east),
            send(ft, fbuf.at[c], 2, north),
            send(fbuf.at[east, first], fbuf.at[east, first], 3, north),
            send(fbuf.at[north, second], fbuf.at[north, second], 4, east),
            send(fbuf.at[east], fbuf.at[east], 5, pair),
            send(fbuf.at[north], fbuf.at[north], 6, pair),
            send(fbuf.at[diagonal], fbuf.at[diagonal], 7, pair),
        ]
        for role in (1, 2, 0):
            sends[role].start()

        def arrived(role):
            place = fbuf.at[slots[role]]
            if role == 3:
                place = fbuf.at[diagonal, first]
            if role == 4:
                place = fbuf.at[diagonal, second]
            send(place, place, role, pair).wait_recv()

    else:
        sends = [send(ft, fbuf.at[c], i, mate) for i, mate in enumerate(mates)]
        for copy in sends:
            copy.start()

    @pl.loop(0, tiles)
    def _(t):
        slot = lax.rem(t, 2)

        @pl.when(t + 1 < tiles)
        def _():
            load(t + 1, 1 - slot).start()

        load(t, slot).wait()
        words[:, pl.ds(pl.multiple_of(t * tile, tile), tile)] = stage[slot].T

    total[...] = jnp.zeros_like(total)
    own.wait()

    def product(slot, start, size):
        packed = words[pl.ds(pl.multiple_of(slot * wide, wide), wide), pl.ds(start, size)]
        return lax.dot_general(
            fbuf[slot], expand_bits(packed), (((1,), (0,)), ((), ())), preferred_element_type=jnp.float32
        )

    early = n_col - 2

    @pl.loop(0, early * halves)
    def _(t):
        step = t // halves
        start = pl.multiple_of(lax.rem(t, halves) * half, half)
        fresh = lax.rem(t, halves) == 0
        if paired:

            @pl.when(jnp.logical_and(fresh, step == 1))
            def _():
                arrived(0)

            @pl.when(jnp.logical_and(fresh, step == 2))
            def _():
                arrived(1)
                sends[3].start()
                sends[5].start()
                arrived(2)
                sends[4].start()
                sends[6].start()

            @pl.when(jnp.logical_and(fresh, step == 4))
            def _():
                arrived(5)

            @pl.when(jnp.logical_and(fresh, step == 5))
            def _():
                arrived(6)
                arrived(3)
                arrived(4)
                sends[7].start()

            slot = c
            for number, choice in enumerate((slots[0], slots[1], slots[2], slots[5], slots[6])):
                slot = jnp.where(step == number + 1, choice, slot)
        else:
            slot = lax.rem(c + n_col - step, n_col)

            @pl.when(jnp.logical_and(fresh, step > 0))
            def _():
                send(fbuf.at[slot], fbuf.at[slot], step - 1, mates[0]).wait_recv()

        total[:, pl.ds(start, half)] += product(slot, start, half)

    if paired:
        arrived(7)
        last = (slots[3], slots[7])
    else:
        last = (lax.rem(c + 2, n_col), lax.rem(c + 1, n_col))
        for slot, role in zip(last, (n_col - 3, n_col - 2)):
            send(fbuf.at[slot], fbuf.at[slot], role, mates[0]).wait_recv()

    def exchange(t, other):
        return pltpu.make_async_remote_copy(
            src_ref=out_code.at[t], dst_ref=in_code.at[t], send_sem=psend.at[t], recv_sem=precv.at[t],
            device_id={"row": other}, device_id_type=MESH,
        )

    @pl.loop(0, n_row)
    def _(t):
        other = lax.rem(r + 1 + t, n_row)
        start = pl.multiple_of(other * part, part)
        block = total[:, pl.ds(start, part)] + product(last[0], start, part)
        block = block + product(last[1], start, part)

        @pl.when(t < n_row - 1)
        def _():
            out_code[t] = encode(block, scale)
            exchange(t, other).start()

        @pl.when(t == n_row - 1)
        def _():
            total[:, pl.ds(0, part)] = block

    def received(t, value):
        exchange(t, others[0]).wait_recv()
        return value + decode(in_code[t], scale)

    reached = total[:, pl.ds(0, part)]
    for t in range(n_row - 1):
        reached = received(t, reached)
    place = lax.broadcasted_iota(jnp.int32, (32, part), 0)
    kept, added = [], []
    for word in range(visited.shape[0]):
        value = reached[word * 32 : word * 32 + 32]
        unseen = ((visited[word : word + 1, :] >> place) & 1) == 0
        kept.append(jnp.where(unseen, value, 0.0))
        marks = jnp.where(jnp.logical_and(unseen, value > 0), jnp.int32(1) << place, 0)
        added.append(jnp.sum(marks, axis=0, keepdims=True))
    counts[...] = jnp.concatenate(kept, axis=0).T
    bits[...] = visited[...] | jnp.concatenate(added, axis=0)
    for copy in sends:
        copy.wait_send()
    for t in range(n_row - 1):
        exchange(t, others[0]).wait_send()


ROLES = 19


def unpack(packed):
    one = jnp.full((32, packed.shape[1]), 1, jnp.float8_e4m3fn)
    zero = jnp.full((32, packed.shape[1]), 0, jnp.float8_e4m3fn)
    pieces = []
    for block in range(packed.shape[0] // 32):
        part = packed[block * 32 : block * 32 + 32]
        for bit in range(8):
            mask = np.int8(-128) if bit == 7 else np.int8(1 << bit)
            pieces.append(jnp.where((part & mask) != 0, one, zero))
    return jnp.concatenate(pieces, axis=0)


def grouped(
    groups, adj, src, own_sum,
    stage, packed_own, packed, own_f, fb, rem, out_code, in_code,
    load_sem, own_sem, fsend, frecv, psend, precv,
):
    n_row, n_col = 4, 8
    r, c = lax.axis_index("row"), lax.axis_index("col")
    dst, width = adj.shape
    depth, roots = src.shape
    part = dst // n_row
    wide = width // n_col * 4
    lanes = width // 4
    tile = dst // 2
    scale = LEVELS / math.log(width * 64 * 1.01 / LOW)
    last = len(groups) - 1
    firsts = [sum(groups[:g]) for g in range(len(groups))]
    pair, east, north = flip(c, 1), flip(c, 2), flip(c, 4)
    diagonal = flip(east, 4)
    slots = [c, pair, east, north, flip(pair, 2), flip(pair, 4), diagonal, flip(diagonal, 1)]
    blocks = [0, 0, 1, 2, 1, 2, 3, 3]
    middle = jnp.logical_or(r == 1, r == 2)
    high = r // 2
    relay = 1 + high
    order = []
    for a, b in zip((3, 2, 1), (2, 3, 0)):
        low = jnp.where(middle, b, a)
        order.append(low + high * (3 - 2 * low))
    senders = [
        jnp.where(middle, 2 - high, 1 + high),
        jnp.where(middle, 3 - 3 * high, 2 - high),
    ]

    def chosen(step, values):
        value = values[0]
        for number in range(1, len(values)):
            value = jnp.where(step == number, values[number], value)
        return value

    barrier = pltpu.get_barrier_semaphore()
    for mate in (pair, east, north):
        pl.semaphore_signal(barrier, inc=1, device_id={"col": mate}, device_id_type=MESH)
    for other in senders:
        pl.semaphore_signal(barrier, inc=1, device_id={"row": other}, device_id_type=MESH)

    @pl.when(middle)
    def _():
        pl.semaphore_signal(barrier, inc=1, device_id={"row": 3 * high}, device_id_type=MESH)

    frontier_copy = pltpu.make_async_copy(src, own_f, own_sem)
    frontier_copy.start()

    def load(b, i):
        lane = pl.multiple_of(chosen(b, [slots[k] // 2 * lanes for k in (0, 2, 3, 6)]), lanes)
        lines = pl.ds(pl.multiple_of(i * tile, tile), tile)
        return pltpu.make_async_copy(
            adj.at[lines, pl.ds(lane, lanes)], stage.at[b, lines], load_sem.at[b, i]
        )

    for b in (0, 1):
        load(b, 0).start()
        load(b, 1).start()

    line = lax.broadcasted_iota(jnp.int32, (256, 256), 0)
    place = lax.broadcasted_iota(jnp.int32, (256, 256), 1)
    target = (line % 8) * 32 + ((line // 8) % 4) * 8 + line // 32
    shuffle = jnp.where(target == place, 1.0, 0.0).astype(jnp.bfloat16)
    frontier_copy.wait()
    for block in range(depth // 256):
        columns = slice(block * 256, block * 256 + 256)
        fb[c, :, columns] = lax.dot_general(
            own_f[columns, :], shuffle, (((0,), (0,)), ((), ())), preferred_element_type=jnp.float32
        ).astype(jnp.bfloat16)

    def rows(g):
        return pl.ds(firsts[g], groups[g])

    def send(ref, g, role, i, mate):
        number = g * ROLES + (0, 1, 5, 9, 9, 13, 15, 17)[role] + i
        return pltpu.make_async_remote_copy(
            src_ref=ref, dst_ref=ref, send_sem=fsend.at[number], recv_sem=frecv.at[number],
            device_id={"col": mate}, device_id_type=MESH,
        )

    def piece(g, role, i, slot):
        size = depth // 4 if role < 5 else depth // 2
        return fb.at[slot, rows(g), pl.ds(i * size, size)]

    def to_pair(g):
        return send(fb.at[c, rows(g)], g, 0, 0, pair)

    def message(g, role, i):
        source, mate = {
            1: (c, east), 2: (c, north), 3: (east, north), 4: (north, east),
            5: (east, pair), 6: (north, pair), 7: (diagonal, pair),
        }[role]
        return send(piece(g, role, i, source), g, role, i, mate)

    def arrived(g, role, i):
        slot = {1: 2, 2: 3, 3: 6, 4: 6, 5: 4, 6: 5, 7: 7}[role]
        send(piece(g, role, i, slots[slot]), g, role, i, pair).wait_recv()

    def first_sends(g):
        for i in range(4):
            message(g, 1, i).start()
            message(g, 2, (i + 2) % 4).start()

    def forward(g, i):
        arrived(g, 1, i)
        message(g, 3, i).start()
        arrived(g, 2, i + 2)
        message(g, 4, i + 2).start()

    def forward_rest(g):
        forward(g, 1)
        if g < last:
            first_sends(g + 1)
        message(g, 5, 0).start()
        message(g, 6, 1).start()

    def share_rest(g):
        arrived(g, 1, 2)
        arrived(g, 1, 3)
        message(g, 5, 1).start()
        arrived(g, 2, 0)
        arrived(g, 2, 1)
        message(g, 6, 0).start()

    def share_diagonal(g):
        arrived(g, 3, 0)
        arrived(g, 3, 1)
        message(g, 7, 0).start()
        arrived(g, 4, 2)
        arrived(g, 4, 3)
        message(g, 7, 1).start()

    pl.semaphore_wait(barrier, 5 + jnp.where(middle, 1, 0))
    first_sends(0)
    for g in range(len(groups)):
        to_pair(g).start()
    for b in (2, 3):
        load(b, 0).start()
        load(b, 1).start()

    def turn(out, b, i):
        columns = pl.ds(pl.multiple_of(i * tile, tile), tile)
        turned = stage[b, columns, :].T.reshape(lanes // 8, 8, tile)
        spread = jnp.concatenate([turned, turned >> 8, turned >> 16, turned >> 24], axis=1)
        target = pl.ds(pl.multiple_of((b - 1) * lanes * 4, lanes * 4), lanes * 4) if out is packed else slice(None)
        out[target, columns] = spread.reshape(lanes * 4, tile).astype(jnp.int8)

    def product(lhs, slot, block, start, size):
        ref, first = (packed, block - 1) if block else (packed_own, 0)
        base = pl.multiple_of(first * lanes * 4 + lax.rem(slot, 2) * wide, wide)
        return lax.dot_general(
            lhs, unpack(ref[pl.ds(base, wide), pl.ds(start, size)]), (((1,), (0,)), ((), ())),
            preferred_element_type=jnp.float32,
        )

    def add_step(span, pairs):
        for t in range(3):
            start = pl.multiple_of(order[t] * part, part)
            value = rem[t, span, :]
            for slot, block in pairs:
                value = value + product(fb[slot, span, :], slot, block, start, part)
            rem[t, span, :] = value

    def exchange(g, t, slot, other):
        return pltpu.make_async_remote_copy(
            src_ref=out_code.at[t, rows(g)], dst_ref=in_code.at[slot, rows(g)], send_sem=psend.at[g, t],
            recv_sem=precv.at[g, slot], device_id={"row": other}, device_id_type=MESH,
        )

    def received(g, slot):
        exchange(g, 0, slot, relay).wait_recv()
        return decode(in_code[slot, rows(g), :], scale)

    def pass_on(g):
        @pl.when(middle)
        def _():
            out_code[1, rows(g), :] = encode(rem[1, rows(g), :] + received(g, n_row), scale)
            exchange(g, 1, r, order[1]).start()

    rem[...] = jnp.zeros_like(rem)

    @pl.loop(0, 2)
    def _(i):
        load(0, i).wait()
        turn(packed_own, 0, i)

    @pl.loop(0, 2)
    def _(step):
        @pl.when(step == 1)
        def _():
            forward(0, 0)
            for g in range(len(groups)):
                send(fb.at[pair, rows(g)], g, 0, 0, pair).wait_recv()

        numbers = [step * 3 + k for k in range(3)]
        for number in numbers:
            load(1 + number // 2, lax.rem(number, 2)).wait()
        add_step(pl.ds(0, roots), [(chosen(step, (c, pair)), 0)])
        for number in numbers:
            turn(packed, 1 + number // 2, lax.rem(number, 2))

    forward_rest(0)

    for g in range(len(groups)):
        share_rest(g)

        @pl.loop(0, 2)
        def _(step):
            @pl.when(step == 1)
            def _():
                share_diagonal(g)
                if 0 < g < last:
                    forward(g + 1, 0)
                for i in (0, 1):
                    arrived(g, 5, i)
                    arrived(g, 6, i)

            add_step(rows(g), [(chosen(step, slots[k : k + 3 : 2]), k - 1) for k in (2, 3)])

        if g == 0 < last:
            forward(1, 0)
        if g:
            pass_on(g - 1)
        if g < last:
            forward_rest(g + 1)
        arrived(g, 7, 0)
        arrived(g, 7, 1)

        @pl.loop(0, 3)
        def _(t):
            target = chosen(t, order)
            start = pl.multiple_of(target * part, part)
            value = rem[t, rows(g), :]
            for slot in slots[6:]:
                value = value + product(fb[slot, rows(g), :], slot, 3, start, part)
            direct = jnp.logical_or(t != 1, jnp.logical_not(middle))

            @pl.when(direct)
            def _():
                out_code[t, rows(g), :] = encode(value, scale)
                first_edge = jnp.logical_and(t == 0, jnp.logical_not(middle))
                exchange(g, t, jnp.where(first_edge, n_row, r), jnp.where(first_edge, relay, target)).start()

            @pl.when(jnp.logical_not(direct))
            def _():
                rem[t, rows(g), :] = value

    quarter = part // 4

    @pl.loop(0, 4)
    def _(q):
        @pl.when(q == 2)
        def _():
            pass_on(last)

        start = pl.multiple_of(r * part + q * quarter, quarter)
        value = jnp.zeros((roots, quarter), jnp.float32)
        for slot, block in zip(slots, blocks):
            value = value + product(fb[slot], slot, block, start, quarter)
        own_sum[:, pl.ds(pl.multiple_of(q * quarter, quarter), quarter)] = value

    for g in range(len(groups)):
        to_pair(g).wait_send()
        for role, places in ((1, 4), (2, 4), (3, 2), (4, 2), (5, 2), (6, 2), (7, 2)):
            for i in range(places):
                message(g, role, i + 2 if role == 4 else i).wait_send()
    for g in range(last):
        for t in range(3):
            exchange(g, t, r, relay).wait_send()
    for g in range(len(groups)):
        for sender in senders:
            own_sum[rows(g), :] += received(g, sender)

        @pl.when(middle)
        def _():
            own_sum[rows(g), :] += received(g, 3 * high)

    for t in range(3):
        exchange(last, t, r, relay).wait_send()


def deliver(reached, visited, counts, bits, held, marked, sem):
    part, roots = held.shape
    size = part // 4

    def copy(i):
        span = pl.ds(i * size, size)
        return pltpu.make_async_copy(held.at[span, :], counts.at[span, :], sem.at[i])

    place = lax.broadcasted_iota(jnp.int32, (32, size), 0)
    for i in range(4):
        span = slice(i * size, i * size + size)
        kept, added = [], []
        for word in range(visited.shape[0]):
            value = reached[word * 32 : word * 32 + 32, span]
            unseen = ((visited[word : word + 1, span] >> place) & 1) == 0
            kept.append(jnp.where(unseen, value, 0.0))
            marks = jnp.where(jnp.logical_and(unseen, value > 0), jnp.int32(1) << place, 0)
            added.append(jnp.sum(marks, axis=0, keepdims=True))
        held[span, :] = jnp.concatenate(kept, axis=0).T
        marked[:, span] = visited[:, span] | jnp.concatenate(added, axis=0)
        if i:
            copy(i - 1).start()
    last = pltpu.make_async_copy(marked, bits, sem.at[4])
    copy(3).start()
    last.start()
    for i in range(4):
        copy(i).wait()
    last.wait()


def grouped_shards(adjacency, frontier, visited):
    dst, width = adjacency.shape
    depth, roots = frontier.shape
    part = dst // 4
    groups = (3 * roots // 8, 3 * roots // 8, roots // 4)
    n_group = len(groups)
    anywhere = pl.BlockSpec(memory_space=pl.ANY)
    vmem = pl.BlockSpec(memory_space=pltpu.VMEM)
    dma = pltpu.SemaphoreType.DMA
    reached = pl.pallas_call(
        functools.partial(grouped, groups),
        out_shape=jax.ShapeDtypeStruct((roots, part), jnp.float32),
        in_specs=[anywhere] * 2,
        out_specs=vmem,
        scratch_shapes=[
            pltpu.VMEM((4, dst, width // 4), jnp.int32),
            pltpu.VMEM((width, dst), jnp.int8),
            pltpu.VMEM((width * 3, dst), jnp.int8),
            pltpu.VMEM((depth, roots), jnp.bfloat16),
            pltpu.VMEM((8, roots, depth), jnp.bfloat16),
            pltpu.VMEM((3, roots, part), jnp.float32),
            pltpu.VMEM((3, roots, part), jnp.int16),
            pltpu.VMEM((5, roots, part), jnp.int16),
            dma((4, 2)),
            dma,
            dma((n_group * ROLES,)),
            dma((n_group * ROLES,)),
            dma((n_group, 3)),
            dma((n_group, 5)),
        ],
        compiler_params=pltpu.CompilerParams(
            collective_id=0, has_side_effects=True, vmem_limit_bytes=53 * 2**20
        ),
    )(adjacency, frontier)
    return pl.pallas_call(
        deliver,
        out_shape=(
            jax.ShapeDtypeStruct((part, roots), jnp.float32),
            jax.ShapeDtypeStruct((visited.shape[0], part), jnp.int32),
        ),
        in_specs=[vmem] * 2,
        out_specs=(anywhere, anywhere),
        scratch_shapes=[
            pltpu.VMEM((part, roots), jnp.float32),
            pltpu.VMEM((visited.shape[0], part), jnp.int32),
            dma((5,)),
        ],
        compiler_params=pltpu.CompilerParams(vmem_limit_bytes=4 * 2**20),
    )(reached, visited)


def shards(n_row, n_col, adjacency, frontier, visited):
    dst, width = adjacency.shape
    depth, roots = frontier.shape
    part = dst // n_row
    tile = math.gcd(dst, 256)
    ft = jnp.transpose(frontier.reshape(depth // 32, 32, roots), (2, 1, 0)).reshape(roots, depth)
    vmem = pl.BlockSpec(memory_space=pltpu.VMEM)
    roles = 8 if n_col == 8 else n_col - 1
    dma = pltpu.SemaphoreType.DMA
    return pl.pallas_call(
        functools.partial(kernel, n_row, n_col),
        out_shape=(
            jax.ShapeDtypeStruct((part, roots), jnp.float32),
            jax.ShapeDtypeStruct((visited.shape[0], part), jnp.int32),
        ),
        in_specs=[pl.BlockSpec(memory_space=pl.ANY), vmem, vmem],
        out_specs=(vmem, vmem),
        scratch_shapes=[
            pltpu.VMEM((2, tile, width), jnp.int32),
            pltpu.VMEM((width, dst), jnp.int32),
            pltpu.VMEM((n_col, roots, depth), jnp.bfloat16),
            pltpu.VMEM((roots, dst), jnp.float32),
            pltpu.VMEM((n_row - 1, roots, part), jnp.int16),
            pltpu.VMEM((n_row - 1, roots, part), jnp.int16),
            dma((2,)),
            dma,
            dma((roles,)),
            dma((roles,)),
            dma((n_row - 1,)),
            dma((n_row - 1,)),
        ],
        compiler_params=pltpu.CompilerParams(
            collective_id=0, has_side_effects=True, vmem_limit_bytes=56 * 2**20
        ),
    )(adjacency, ft, visited)


def solution(mesh):
    placed = (P("col", "row"), P(("row", "col"), None), P(None, ("col", "row")))
    n_row, n_col = mesh.shape["row"], mesh.shape["col"]
    body = grouped_shards if (n_row, n_col) == (4, 8) else functools.partial(shards, n_row, n_col)
    return jax.shard_map(
        body,
        mesh=mesh,
        in_specs=placed,
        out_specs=(P(("col", "row"), None), P(None, ("col", "row"))),
        check_vma=False,
    )
```

```python
import functools
import math

import jax
import jax.numpy as jnp
import numpy as np
from jax import lax
from jax.experimental import pallas as pl
from jax.experimental.pallas import tpu as pltpu
from jax.sharding import PartitionSpec as P

MESH = pl.DeviceIdType.MESH
LOW = 0.09
LEVELS = 65000.0


def expand_bits(words):
    one = jnp.full(words.shape, 1, jnp.float8_e4m3fn)
    zero = jnp.full(words.shape, 0, jnp.float8_e4m3fn)
    pieces = []
    for byte in range(4):
        part = (words >> (8 * byte)).astype(jnp.int8)
        for bit in range(8):
            mask = np.int8(-128) if bit == 7 else np.int8(1 << bit)
            pieces.append(jnp.where((part & mask) != 0, one, zero))
    return jnp.concatenate(pieces, axis=0)


def encode(value, scale):
    code = jnp.log(jnp.maximum(value, LOW)) * scale + (1.5 - math.log(LOW) * scale)
    code = jnp.where(value > 0, code, 0.0).astype(jnp.int32)
    return (code - 32768).astype(jnp.int16)


def decode(code, scale):
    code = code.astype(jnp.int32) + 32768
    value = jnp.exp((code - 1).astype(jnp.float32) * (1.0 / scale) + math.log(LOW))
    return jnp.where(code > 0, value, 0.0)


def flip(index, bit):
    return index + bit - 2 * bit * ((index // bit) % 2)


def kernel(
    n_row, n_col, adj, ft, visited, counts, bits,
    stage, words, fbuf, total, out_code, in_code,
    load_sem, own_sem, fsend, frecv, psend, precv,
):
    r, c = lax.axis_index("row"), lax.axis_index("col")
    dst, width = adj.shape
    depth = ft.shape[1]
    wide = width // n_col
    part = dst // n_row
    half = math.gcd(dst, 2048)
    halves = dst // half
    tile = stage.shape[1]
    tiles = dst // tile
    paired = n_col == 8
    scale = LEVELS / math.log(width * 32 * 1.01 / LOW)

    def load(t, slot):
        return pltpu.make_async_copy(
            adj.at[pl.ds(pl.multiple_of(t * tile, tile), tile), :], stage.at[slot], load_sem.at[slot]
        )

    load(0, 0).start()
    own = pltpu.make_async_copy(ft, fbuf.at[c], own_sem)
    own.start()

    if paired:
        mates = [flip(c, 1), flip(c, 2), flip(c, 4)]
    else:
        mates = [lax.rem(c + i, n_col) for i in range(1, n_col)]
    others = [lax.rem(r + i, n_row) for i in range(1, n_row)]
    barrier = pltpu.get_barrier_semaphore()
    for mate in mates:
        pl.semaphore_signal(barrier, inc=1, device_id={"col": mate}, device_id_type=MESH)
    for other in others:
        pl.semaphore_signal(barrier, inc=1, device_id={"row": other}, device_id_type=MESH)
    pl.semaphore_wait(barrier, len(mates) + len(others))

    def send(src, dst_ref, role, mate):
        return pltpu.make_async_remote_copy(
            src_ref=src, dst_ref=dst_ref, send_sem=fsend.at[role], recv_sem=frecv.at[role],
            device_id={"col": mate}, device_id_type=MESH,
        )

    if paired:
        pair, east, north = mates
        first, second = pl.ds(0, ft.shape[0] // 2), pl.ds(ft.shape[0] // 2, ft.shape[0] // 2)
        diagonal = flip(east, 4)
        slots = [pair, east, north, diagonal, diagonal, flip(pair, 2), flip(pair, 4), flip(diagonal, 1)]
        sends = [
            send(ft, fbuf.at[c], 0, pair),
            send(ft, fbuf.at[c], 1, east),
            send(ft, fbuf.at[c], 2, north),
            send(fbuf.at[east, first], fbuf.at[east, first], 3, north),
            send(fbuf.at[north, second], fbuf.at[north, second], 4, east),
            send(fbuf.at[east], fbuf.at[east], 5, pair),
            send(fbuf.at[north], fbuf.at[north], 6, pair),
            send(fbuf.at[diagonal], fbuf.at[diagonal], 7, pair),
        ]
        for role in (1, 2, 0):
            sends[role].start()

        def arrived(role):
            place = fbuf.at[slots[role]]
            if role == 3:
                place = fbuf.at[diagonal, first]
            if role == 4:
                place = fbuf.at[diagonal, second]
            send(place, place, role, pair).wait_recv()

    else:
        sends = [send(ft, fbuf.at[c], i, mate) for i, mate in enumerate(mates)]
        for copy in sends:
            copy.start()

    @pl.loop(0, tiles)
    def _(t):
        slot = lax.rem(t, 2)

        @pl.when(t + 1 < tiles)
        def _():
            load(t + 1, 1 - slot).start()

        load(t, slot).wait()
        words[:, pl.ds(pl.multiple_of(t * tile, tile), tile)] = stage[slot].T

    total[...] = jnp.zeros_like(total)
    own.wait()

    def product(slot, start, size):
        packed = words[pl.ds(pl.multiple_of(slot * wide, wide), wide), pl.ds(start, size)]
        return lax.dot_general(
            fbuf[slot], expand_bits(packed), (((1,), (0,)), ((), ())), preferred_element_type=jnp.float32
        )

    early = n_col - 2

    @pl.loop(0, early * halves)
    def _(t):
        step = t // halves
        start = pl.multiple_of(lax.rem(t, halves) * half, half)
        fresh = lax.rem(t, halves) == 0
        if paired:

            @pl.when(jnp.logical_and(fresh, step == 1))
            def _():
                arrived(0)

            @pl.when(jnp.logical_and(fresh, step == 2))
            def _():
                arrived(1)
                sends[3].start()
                sends[5].start()
                arrived(2)
                sends[4].start()
                sends[6].start()

            @pl.when(jnp.logical_and(fresh, step == 4))
            def _():
                arrived(5)

            @pl.when(jnp.logical_and(fresh, step == 5))
            def _():
                arrived(6)
                arrived(3)
                arrived(4)
                sends[7].start()

            slot = c
            for number, choice in enumerate((slots[0], slots[1], slots[2], slots[5], slots[6])):
                slot = jnp.where(step == number + 1, choice, slot)
        else:
            slot = lax.rem(c + n_col - step, n_col)

            @pl.when(jnp.logical_and(fresh, step > 0))
            def _():
                send(fbuf.at[slot], fbuf.at[slot], step - 1, mates[0]).wait_recv()

        total[:, pl.ds(start, half)] += product(slot, start, half)

    if paired:
        arrived(7)
        last = (slots[3], slots[7])
    else:
        last = (lax.rem(c + 2, n_col), lax.rem(c + 1, n_col))
        for slot, role in zip(last, (n_col - 3, n_col - 2)):
            send(fbuf.at[slot], fbuf.at[slot], role, mates[0]).wait_recv()

    def exchange(t, other):
        return pltpu.make_async_remote_copy(
            src_ref=out_code.at[t], dst_ref=in_code.at[t], send_sem=psend.at[t], recv_sem=precv.at[t],
            device_id={"row": other}, device_id_type=MESH,
        )

    @pl.loop(0, n_row)
    def _(t):
        other = lax.rem(r + 1 + t, n_row)
        start = pl.multiple_of(other * part, part)
        block = total[:, pl.ds(start, part)] + product(last[0], start, part)
        block = block + product(last[1], start, part)

        @pl.when(t < n_row - 1)
        def _():
            out_code[t] = encode(block, scale)
            exchange(t, other).start()

        @pl.when(t == n_row - 1)
        def _():
            total[:, pl.ds(0, part)] = block

    def received(t, value):
        exchange(t, others[0]).wait_recv()
        return value + decode(in_code[t], scale)

    reached = total[:, pl.ds(0, part)]
    for t in range(n_row - 1):
        reached = received(t, reached)
    place = lax.broadcasted_iota(jnp.int32, (32, part), 0)
    kept, added = [], []
    for word in range(visited.shape[0]):
        value = reached[word * 32 : word * 32 + 32]
        unseen = ((visited[word : word + 1, :] >> place) & 1) == 0
        kept.append(jnp.where(unseen, value, 0.0))
        marks = jnp.where(jnp.logical_and(unseen, value > 0), jnp.int32(1) << place, 0)
        added.append(jnp.sum(marks, axis=0, keepdims=True))
    counts[...] = jnp.concatenate(kept, axis=0).T
    bits[...] = visited[...] | jnp.concatenate(added, axis=0)
    for copy in sends:
        copy.wait_send()
    for t in range(n_row - 1):
        exchange(t, others[0]).wait_send()


ROLES = 19


def unpack(packed):
    one = jnp.full((32, packed.shape[1]), 1, jnp.float8_e4m3fn)
    zero = jnp.full((32, packed.shape[1]), 0, jnp.float8_e4m3fn)
    pieces = []
    for block in range(packed.shape[0] // 32):
        part = packed[block * 32 : block * 32 + 32]
        for bit in range(8):
            mask = np.int8(-128) if bit == 7 else np.int8(1 << bit)
            pieces.append(jnp.where((part & mask) != 0, one, zero))
    return jnp.concatenate(pieces, axis=0)


def grouped(
    groups, adj, src, own_sum,
    stage, packed_own, packed, own_f, fb, rem, out_code, in_code,
    load_sem, own_sem, fsend, frecv, psend, precv,
):
    n_row, n_col = 4, 8
    r, c = lax.axis_index("row"), lax.axis_index("col")
    dst, width = adj.shape
    depth, roots = src.shape
    part = dst // n_row
    wide = width // n_col * 4
    lanes = width // 4
    tile = dst // 2
    scale = LEVELS / math.log(width * 64 * 1.01 / LOW)
    last = len(groups) - 1
    firsts = [sum(groups[:g]) for g in range(len(groups))]
    pair, east, north = flip(c, 1), flip(c, 2), flip(c, 4)
    diagonal = flip(east, 4)
    slots = [c, pair, east, north, flip(pair, 2), flip(pair, 4), diagonal, flip(diagonal, 1)]
    blocks = [0, 0, 1, 2, 1, 2, 3, 3]
    middle = jnp.logical_or(r == 1, r == 2)
    high = r // 2
    relay = 1 + high
    order = []
    for a, b in zip((3, 2, 1), (2, 3, 0)):
        low = jnp.where(middle, b, a)
        order.append(low + high * (3 - 2 * low))
    senders = [
        jnp.where(middle, 2 - high, 1 + high),
        jnp.where(middle, 3 - 3 * high, 2 - high),
    ]

    def chosen(step, values):
        value = values[0]
        for number in range(1, len(values)):
            value = jnp.where(step == number, values[number], value)
        return value

    barrier = pltpu.get_barrier_semaphore()
    for mate in (pair, east, north):
        pl.semaphore_signal(barrier, inc=1, device_id={"col": mate}, device_id_type=MESH)
    for other in senders:
        pl.semaphore_signal(barrier, inc=1, device_id={"row": other}, device_id_type=MESH)

    @pl.when(middle)
    def _():
        pl.semaphore_signal(barrier, inc=1, device_id={"row": 3 * high}, device_id_type=MESH)

    frontier_copy = pltpu.make_async_copy(src, own_f, own_sem)
    frontier_copy.start()

    def load(b, i):
        lane = pl.multiple_of(chosen(b, [slots[k] // 2 * lanes for k in (0, 2, 3, 6)]), lanes)
        lines = pl.ds(pl.multiple_of(i * tile, tile), tile)
        return pltpu.make_async_copy(
            adj.at[lines, pl.ds(lane, lanes)], stage.at[b, lines], load_sem.at[b, i]
        )

    for b in (0, 1):
        load(b, 0).start()
        load(b, 1).start()

    line = lax.broadcasted_iota(jnp.int32, (256, 256), 0)
    place = lax.broadcasted_iota(jnp.int32, (256, 256), 1)
    target = (line % 8) * 32 + ((line // 8) % 4) * 8 + line // 32
    shuffle = jnp.where(target == place, 1.0, 0.0).astype(jnp.bfloat16)
    frontier_copy.wait()
    for block in range(depth // 256):
        columns = slice(block * 256, block * 256 + 256)
        fb[c, :, columns] = lax.dot_general(
            own_f[columns, :], shuffle, (((0,), (0,)), ((), ())), preferred_element_type=jnp.float32
        ).astype(jnp.bfloat16)

    def rows(g):
        return pl.ds(firsts[g], groups[g])

    def send(ref, g, role, i, mate):
        number = g * ROLES + (0, 1, 5, 9, 9, 13, 15, 17)[role] + i
        return pltpu.make_async_remote_copy(
            src_ref=ref, dst_ref=ref, send_sem=fsend.at[number], recv_sem=frecv.at[number],
            device_id={"col": mate}, device_id_type=MESH,
        )

    def piece(g, role, i, slot):
        size = depth // 4 if role < 5 else depth // 2
        return fb.at[slot, rows(g), pl.ds(i * size, size)]

    def to_pair(g):
        return send(fb.at[c, rows(g)], g, 0, 0, pair)

    def message(g, role, i):
        source, mate = {
            1: (c, east), 2: (c, north), 3: (east, north), 4: (north, east),
            5: (east, pair), 6: (north, pair), 7: (diagonal, pair),
        }[role]
        return send(piece(g, role, i, source), g, role, i, mate)

    def arrived(g, role, i):
        slot = {1: 2, 2: 3, 3: 6, 4: 6, 5: 4, 6: 5, 7: 7}[role]
        send(piece(g, role, i, slots[slot]), g, role, i, pair).wait_recv()

    def first_sends(g):
        for i in range(4):
            message(g, 1, i).start()
            message(g, 2, (i + 2) % 4).start()

    def forward(g, i):
        arrived(g, 1, i)
        message(g, 3, i).start()
        arrived(g, 2, i + 2)
        message(g, 4, i + 2).start()

    def forward_rest(g):
        forward(g, 1)
        if g < last:
            first_sends(g + 1)
        message(g, 5, 0).start()
        message(g, 6, 1).start()

    def share_rest(g):
        arrived(g, 1, 2)
        arrived(g, 1, 3)
        message(g, 5, 1).start()
        arrived(g, 2, 0)
        arrived(g, 2, 1)
        message(g, 6, 0).start()

    def share_diagonal(g):
        arrived(g, 3, 0)
        arrived(g, 3, 1)
        message(g, 7, 0).start()
        arrived(g, 4, 2)
        arrived(g, 4, 3)
        message(g, 7, 1).start()

    pl.semaphore_wait(barrier, 5 + jnp.where(middle, 1, 0))
    first_sends(0)
    for g in range(len(groups)):
        to_pair(g).start()
    for b in (2, 3):
        load(b, 0).start()
        load(b, 1).start()

    def turn(out, b, i):
        columns = pl.ds(pl.multiple_of(i * tile, tile), tile)
        turned = stage[b, columns, :].T.reshape(lanes // 8, 8, tile)
        spread = jnp.concatenate([turned, turned >> 8, turned >> 16, turned >> 24], axis=1)
        target = pl.ds(pl.multiple_of((b - 1) * lanes * 4, lanes * 4), lanes * 4) if out is packed else slice(None)
        out[target, columns] = spread.reshape(lanes * 4, tile).astype(jnp.int8)

    def product(lhs, slot, block, start, size):
        ref, first = (packed, block - 1) if block else (packed_own, 0)
        base = pl.multiple_of(first * lanes * 4 + lax.rem(slot, 2) * wide, wide)
        return lax.dot_general(
            lhs, unpack(ref[pl.ds(base, wide), pl.ds(start, size)]), (((1,), (0,)), ((), ())),
            preferred_element_type=jnp.float32,
        )

    def add_step(span, pairs):
        for t in range(3):
            start = pl.multiple_of(order[t] * part, part)
            value = rem[t, span, :]
            for slot, block in pairs:
                value = value + product(fb[slot, span, :], slot, block, start, part)
            rem[t, span, :] = value

    def exchange(g, t, slot, other):
        return pltpu.make_async_remote_copy(
            src_ref=out_code.at[t, rows(g)], dst_ref=in_code.at[slot, rows(g)], send_sem=psend.at[g, t],
            recv_sem=precv.at[g, slot], device_id={"row": other}, device_id_type=MESH,
        )

    def received(g, slot):
        exchange(g, 0, slot, relay).wait_recv()
        return decode(in_code[slot, rows(g), :], scale)

    def pass_on(g):
        @pl.when(middle)
        def _():
            out_code[1, rows(g), :] = encode(rem[1, rows(g), :] + received(g, n_row), scale)
            exchange(g, 1, r, order[1]).start()

    rem[...] = jnp.zeros_like(rem)

    @pl.loop(0, 2)
    def _(i):
        load(0, i).wait()
        turn(packed_own, 0, i)

    @pl.loop(0, 2)
    def _(step):
        @pl.when(step == 1)
        def _():
            forward(0, 0)
            for g in range(len(groups)):
                send(fb.at[pair, rows(g)], g, 0, 0, pair).wait_recv()

        numbers = [step * 3 + k for k in range(3)]
        for number in numbers:
            load(1 + number // 2, lax.rem(number, 2)).wait()
        add_step(pl.ds(0, roots), [(chosen(step, (c, pair)), 0)])
        for number in numbers:
            turn(packed, 1 + number // 2, lax.rem(number, 2))

    forward_rest(0)

    for g in range(len(groups)):
        share_rest(g)

        @pl.loop(0, 2)
        def _(step):
            @pl.when(step == 1)
            def _():
                share_diagonal(g)
                if 0 < g < last:
                    pass_on(g - 1)
                    forward(g + 1, 0)
                for i in (0, 1):
                    arrived(g, 5, i)
                    arrived(g, 6, i)

            add_step(rows(g), [(chosen(step, slots[k : k + 3 : 2]), k - 1) for k in (2, 3)])

        if g == 0 < last:
            forward(1, 0)
        if g == last > 0:
            pass_on(g - 1)
        if g < last:
            forward_rest(g + 1)
        arrived(g, 7, 0)
        arrived(g, 7, 1)

        @pl.loop(0, 3)
        def _(t):
            target = chosen(t, order)
            start = pl.multiple_of(target * part, part)
            value = rem[t, rows(g), :]
            for slot in slots[6:]:
                value = value + product(fb[slot, rows(g), :], slot, 3, start, part)
            direct = jnp.logical_or(t != 1, jnp.logical_not(middle))

            @pl.when(direct)
            def _():
                out_code[t, rows(g), :] = encode(value, scale)
                first_edge = jnp.logical_and(t == 0, jnp.logical_not(middle))
                exchange(g, t, jnp.where(first_edge, n_row, r), jnp.where(first_edge, relay, target)).start()

            @pl.when(jnp.logical_not(direct))
            def _():
                rem[t, rows(g), :] = value

    quarter = part // 4

    @pl.loop(0, 4)
    def _(q):
        @pl.when(q == 2)
        def _():
            pass_on(last)

        start = pl.multiple_of(r * part + q * quarter, quarter)
        value = jnp.zeros((roots, quarter), jnp.float32)
        for slot, block in zip(slots, blocks):
            value = value + product(fb[slot], slot, block, start, quarter)
        own_sum[:, pl.ds(pl.multiple_of(q * quarter, quarter), quarter)] = value

    for g in range(len(groups)):
        to_pair(g).wait_send()
        for role, places in ((1, 4), (2, 4), (3, 2), (4, 2), (5, 2), (6, 2), (7, 2)):
            for i in range(places):
                message(g, role, i + 2 if role == 4 else i).wait_send()
    for g in range(last):
        for t in range(3):
            exchange(g, t, r, relay).wait_send()
    for g in range(len(groups)):
        for sender in senders:
            own_sum[rows(g), :] += received(g, sender)

        @pl.when(middle)
        def _():
            own_sum[rows(g), :] += received(g, 3 * high)

    for t in range(3):
        exchange(last, t, r, relay).wait_send()


def deliver(reached, visited, counts, bits, held, marked, sem):
    part, roots = held.shape
    size = part // 4

    def copy(i):
        span = pl.ds(i * size, size)
        return pltpu.make_async_copy(held.at[span, :], counts.at[span, :], sem.at[i])

    place = lax.broadcasted_iota(jnp.int32, (32, size), 0)
    for i in range(4):
        span = slice(i * size, i * size + size)
        kept, added = [], []
        for word in range(visited.shape[0]):
            value = reached[word * 32 : word * 32 + 32, span]
            unseen = ((visited[word : word + 1, span] >> place) & 1) == 0
            kept.append(jnp.where(unseen, value, 0.0))
            marks = jnp.where(jnp.logical_and(unseen, value > 0), jnp.int32(1) << place, 0)
            added.append(jnp.sum(marks, axis=0, keepdims=True))
        held[span, :] = jnp.concatenate(kept, axis=0).T
        marked[:, span] = visited[:, span] | jnp.concatenate(added, axis=0)
        if i:
            copy(i - 1).start()
    last = pltpu.make_async_copy(marked, bits, sem.at[4])
    copy(3).start()
    last.start()
    for i in range(4):
        copy(i).wait()
    last.wait()


def grouped_shards(adjacency, frontier, visited):
    dst, width = adjacency.shape
    depth, roots = frontier.shape
    part = dst // 4
    groups = (3 * roots // 8, 3 * roots // 8, roots // 4)
    n_group = len(groups)
    anywhere = pl.BlockSpec(memory_space=pl.ANY)
    vmem = pl.BlockSpec(memory_space=pltpu.VMEM)
    dma = pltpu.SemaphoreType.DMA
    reached = pl.pallas_call(
        functools.partial(grouped, groups),
        out_shape=jax.ShapeDtypeStruct((roots, part), jnp.float32),
        in_specs=[anywhere] * 2,
        out_specs=vmem,
        scratch_shapes=[
            pltpu.VMEM((4, dst, width // 4), jnp.int32),
            pltpu.VMEM((width, dst), jnp.int8),
            pltpu.VMEM((width * 3, dst), jnp.int8),
            pltpu.VMEM((depth, roots), jnp.bfloat16),
            pltpu.VMEM((8, roots, depth), jnp.bfloat16),
            pltpu.VMEM((3, roots, part), jnp.float32),
            pltpu.VMEM((3, roots, part), jnp.int16),
            pltpu.VMEM((5, roots, part), jnp.int16),
            dma((4, 2)),
            dma,
            dma((n_group * ROLES,)),
            dma((n_group * ROLES,)),
            dma((n_group, 3)),
            dma((n_group, 5)),
        ],
        compiler_params=pltpu.CompilerParams(
            collective_id=0, has_side_effects=True, vmem_limit_bytes=53 * 2**20
        ),
    )(adjacency, frontier)
    return pl.pallas_call(
        deliver,
        out_shape=(
            jax.ShapeDtypeStruct((part, roots), jnp.float32),
            jax.ShapeDtypeStruct((visited.shape[0], part), jnp.int32),
        ),
        in_specs=[vmem] * 2,
        out_specs=(anywhere, anywhere),
        scratch_shapes=[
            pltpu.VMEM((part, roots), jnp.float32),
            pltpu.VMEM((visited.shape[0], part), jnp.int32),
            dma((5,)),
        ],
        compiler_params=pltpu.CompilerParams(vmem_limit_bytes=4 * 2**20),
    )(reached, visited)


def shards(n_row, n_col, adjacency, frontier, visited):
    dst, width = adjacency.shape
    depth, roots = frontier.shape
    part = dst // n_row
    tile = math.gcd(dst, 256)
    ft = jnp.transpose(frontier.reshape(depth // 32, 32, roots), (2, 1, 0)).reshape(roots, depth)
    vmem = pl.BlockSpec(memory_space=pltpu.VMEM)
    roles = 8 if n_col == 8 else n_col - 1
    dma = pltpu.SemaphoreType.DMA
    return pl.pallas_call(
        functools.partial(kernel, n_row, n_col),
        out_shape=(
            jax.ShapeDtypeStruct((part, roots), jnp.float32),
            jax.ShapeDtypeStruct((visited.shape[0], part), jnp.int32),
        ),
        in_specs=[pl.BlockSpec(memory_space=pl.ANY), vmem, vmem],
        out_specs=(vmem, vmem),
        scratch_shapes=[
            pltpu.VMEM((2, tile, width), jnp.int32),
            pltpu.VMEM((width, dst), jnp.int32),
            pltpu.VMEM((n_col, roots, depth), jnp.bfloat16),
            pltpu.VMEM((roots, dst), jnp.float32),
            pltpu.VMEM((n_row - 1, roots, part), jnp.int16),
            pltpu.VMEM((n_row - 1, roots, part), jnp.int16),
            dma((2,)),
            dma,
            dma((roles,)),
            dma((roles,)),
            dma((n_row - 1,)),
            dma((n_row - 1,)),
        ],
        compiler_params=pltpu.CompilerParams(
            collective_id=0, has_side_effects=True, vmem_limit_bytes=56 * 2**20
        ),
    )(adjacency, ft, visited)


def solution(mesh):
    placed = (P("col", "row"), P(("row", "col"), None), P(None, ("col", "row")))
    n_row, n_col = mesh.shape["row"], mesh.shape["col"]
    body = grouped_shards if (n_row, n_col) == (4, 8) else functools.partial(shards, n_row, n_col)
    return jax.shard_map(
        body,
        mesh=mesh,
        in_specs=placed,
        out_specs=(P(("col", "row"), None), P(None, ("col", "row"))),
        check_vma=False,
    )
```
